32 devices in a mesh: lat: 4 (over y, x), lon: 4 (over z), mem: 2 (over core).
Axes of the slice: x: 2, y: 2, z: 4, core: 2. Of those that a mesh axis runs over, the one named last changes fastest.
Arguments:
- anomalies: bfloat16 [24, 4, 1440, 512], P('mem', None, 'lon', 'lat'), may hold values from -6 to 6
- taper: float32 [4, 1440, 512], P('lon', 'lat'), may hold values from 0.5 to 8
- obs_row: int32 [256, 512], P('lat', 'lon'), may hold values from 0 to 511, as said below
- obs_col: int32 [256, 512], P('lat', 'lon'), may hold values from 0 to 1439, as said below
- obs_level: int32 [256, 512], P('lat', 'lon'), may hold values from 0 to 3
- obs_value: float32 [256, 512], P('lat', 'lon'), may hold values from -18 to 18
Outputs:
- increment: float32 [4, 1440, 512], P(None, 'lon', 'lat')
The draws below stay inside these ranges and needn't reach their ends.
Inputs may be any that keep to these rules, and one draw needn't show every extreme that they name: `obs_row`: the entry in row i lies in latitude rows (i // 64) * 128 to (i // 64 + 1) * 128 - 1, drawn evenly there. `obs_col`: the entry in column j lies in longitude columns (j // 128) * 360 to (j // 128 + 1) * 360 - 1, drawn evenly there.
All inputs are finite; a program needn't handle non-finite values.
Results may differ from the reference program's by a relative error of at most 0.0066.
Values may be sent and summed in bfloat16 or wider, within the bound.
A program may use at most 128 MiB of HBM per device.

```python
import math
import jax
import jax.numpy as jnp
from jax import lax

NLAT = 512
NLON = 1440
OBS_BLK = 64
L = 4
M = 24
ROWS_DEV = 128
COLS_DEV = 360
OBS_LAT = 256
OBS_LON = 512


def draw_obs_row(key, part):
    blocks = jnp.arange(OBS_LAT, dtype=jnp.int32)[:, None] // OBS_BLK
    offsets = jax.random.randint(jax.random.fold_in(key, 11), (OBS_LAT, OBS_LON), 0, ROWS_DEV, dtype=jnp.int32)
    return (blocks * ROWS_DEV + offsets).astype(jnp.int32)


def draw_obs_col(key, part):
    blocks = jnp.arange(OBS_LON, dtype=jnp.int32)[None, :] // 128
    offsets = jax.random.randint(jax.random.fold_in(key, 23), (OBS_LAT, OBS_LON), 0, COLS_DEV, dtype=jnp.int32)
    return (blocks * COLS_DEV + offsets).astype(jnp.int32)


def touch_ends(array, own_key, smallest, high):
    longest = array.shape.index(max(array.shape))
    spots = []
    for shift in (0, 1):
        where = [jax.random.randint(jax.random.fold_in(own_key, axis), (), 0, length) for axis, length in enumerate(array.shape)]
        where[longest] = (where[longest] + shift) % array.shape[longest]
        spots.append(tuple(where))
    return array.at[spots[0]].set(smallest).at[spots[1]].set(high)


def shard_levels(rng, extent, cuts, least, top_value):
    def one(dim, parts):
        heights = jax.random.uniform(jax.random.fold_in(jax.random.fold_in(rng, 6), dim), (parts,), jnp.float32, least / len(cuts), top_value / len(cuts))
        return jnp.repeat(jnp.exp(heights), extent[dim] // parts).reshape((-1,) + (1,) * (len(extent) - dim - 1))

    level = one(*cuts[0])
    for cut in cuts[1:]:
        level = level * one(*cut)
    return level


def centred(key, shape, spread, most, shards=(), held_as=jnp.bfloat16):
    level = shard_levels(key, shape, shards, -0.22, 0.18) if shards else 1.0
    entries = jax.random.normal(key, shape, jnp.float32) * spread * level
    return jnp.minimum(jnp.maximum(entries, -most), most).astype(held_as)


def setup_inputs(seed: int = 0) -> dict:
    streams_of = jax.random.split(jax.random.key(seed), 7)
    return {
        "anomalies": centred(streams_of[0], (M, L, NLON, NLAT), 1.0, 6.0, ((0, 2), (2, 4), (3, 4))),
        "taper": jnp.clip(jnp.exp(math.log(8.0) - 2.7725887 * jax.random.uniform(streams_of[1], (L, NLON, NLAT), jnp.float32) ** shard_levels(streams_of[1], (L, NLON, NLAT), ((0, 4), (1, 4)), -0.2, 0.2)), 0.5, 8.0),
        "obs_row": draw_obs_row(jax.random.fold_in(streams_of[6], 71), 0),
        "obs_col": draw_obs_col(jax.random.fold_in(streams_of[6], 71), 0),
        "obs_level": touch_ends(jax.random.randint(streams_of[4], (OBS_LAT, OBS_LON), 0, L), jax.random.fold_in(streams_of[4], 1), 0, L - 1).astype(jnp.int32),
        "obs_value": centred(streams_of[5], (OBS_LAT, OBS_LON), 3.0, 18.0, ((0, 4), (1, 4)), jnp.float32),
    }


def lon_basis(length):
    grid_idx = jnp.arange(length, dtype=jnp.int32)[:, None]
    coef_idx = jnp.arange(length, dtype=jnp.int32)[None, :]
    nyquist = length // 2
    wavenum = jnp.where(coef_idx <= nyquist, coef_idx, coef_idx - nyquist)
    phase_idx = grid_idx * wavenum % length
    angles = phase_idx.astype(jnp.float32) * (2.0 * math.pi / length)
    scales = jnp.where((coef_idx == 0) | (coef_idx == nyquist), 1.0 / math.sqrt(length), math.sqrt(2.0 / length))
    basis = jnp.where(coef_idx <= nyquist, jnp.cos(angles), jnp.sin(angles)) * scales
    return basis.astype(jnp.bfloat16)

def lat_basis(length):
    grid_idx = jnp.arange(length, dtype=jnp.int32)[:, None]
    mode_idx = jnp.arange(length, dtype=jnp.int32)[None, :]
    phase_idx = mode_idx * (2 * grid_idx + 1) % (4 * length)
    angles = phase_idx.astype(jnp.float32) * (math.pi / (2.0 * length))
    scales = jnp.where(mode_idx == 0, 1.0 / math.sqrt(length), math.sqrt(2.0 / length))
    return (jnp.cos(angles) * scales).astype(jnp.bfloat16)

def rounded(value):
    return lax.optimization_barrier(value.astype(jnp.bfloat16)).astype(jnp.float32)

def reference(anomalies, taper, obs_row, obs_col, obs_level, obs_value):
    innovation = jnp.zeros((L, NLON, NLAT), jnp.float32).at[obs_level, obs_col, obs_row].add(obs_value)
    innov_wide = rounded(innovation)
    lon_table = lon_basis(NLON).astype(jnp.float32)
    lat_table = lat_basis(NLAT).astype(jnp.float32)

    def accumulate(summed, member):
        member_wide = member.astype(jnp.float32)
        weighted = rounded(member_wide * innov_wide)
        zonal_coef = rounded(jnp.einsum('lxy,xk->lky', weighted, lon_table))
        spectrum = jnp.einsum('lky,yn->lkn', zonal_coef, lat_table)
        tapered = rounded(spectrum * taper)
        inverse = rounded(jnp.einsum('lkn,yn->lky', tapered, lat_table))
        localized = jnp.einsum('lky,xk->lxy', inverse, lon_table)
        return (summed + member_wide * localized, None)
    summed, _ = lax.scan(accumulate, jnp.zeros((L, NLON, NLAT), jnp.float32), anomalies)
    return summed / (M - 1)
```

```python
import functools
import math

import jax
import jax.numpy as jnp
import numpy as np
from jax import lax
from jax.experimental import pallas as pl
from jax.experimental.pallas import tpu as pltpu
from jax.sharding import PartitionSpec as P


def lon_seeds(block_count, block_size, part_count, part_size):
    length = block_count * block_size
    nyquist = length // 2
    inner = 24 if block_size % 24 == 0 else next(n for n in range(32, 0, -1) if block_size % n == 0)
    outer = block_size // inner
    coef_idx = np.arange(length).reshape(part_count, part_size)
    wavenum = np.where(coef_idx <= nyquist, coef_idx, coef_idx - nyquist)

    def waves(points):
        angles = (points[None, :, None] * wavenum[:, None, :] % length) * (2.0 * math.pi / length)
        return np.cos(angles), np.sin(angles)

    scales = np.where((coef_idx == 0) | (coef_idx == nyquist), 1.0 / math.sqrt(length), math.sqrt(2.0 / length))
    start_cos, start_sin = waves(np.arange(block_count) * block_size)
    is_cos = (coef_idx <= nyquist)[:, None, :]
    first = np.where(is_cos, start_cos, start_sin) * scales[:, None, :]
    second = np.where(is_cos, -start_sin, start_cos) * scales[:, None, :]
    coarse = np.stack([first, second], axis=2).transpose(1, 0, 2, 3)
    high = np.stack(waves(np.arange(outer) * inner))
    low = np.stack(waves(np.arange(inner)))
    return [jnp.asarray(part, jnp.float32) for part in (coarse, high, low)]


def lat_seeds(length):
    inner = next(size for size in range(32, 0, -1) if length % size == 0)
    outer = length // inner
    mode_idx = np.arange(length)[None, :]

    def waves(points):
        angles = (mode_idx * points[:, None] % (4 * length)) * (math.pi / (2.0 * length))
        return np.cos(angles), np.sin(angles)

    scales = np.where(mode_idx == 0, 1.0 / math.sqrt(length), math.sqrt(2.0 / length))
    high = np.stack(waves(np.arange(outer) * (2 * inner))) * scales
    low = np.stack(waves(np.arange(inner) * 2 + 1))
    return [jnp.asarray(part, jnp.float32) for part in (high, low)]


def fused_kernel(
    lat_size, lon_size, own, obs_rows,
    anom, taper, level, column, row, value, coarse, lon_high, lon_low, lat_high, lat_low, out,
    fields, table_fwd, table_inv, fine, modes, taper_near, taper_all, hits, innov_own, innov_all,
    weighted, spectrum, inverse, total, partner_part, lat_send, lat_recv, lon_send, lon_recv,
    level_near, column_near, row_near, value_near, coarse_near, high_near, low_near, lat_high_near, lat_low_near,
    field_ss, field_rs, local_sem, table_sem, taper_ss, taper_rs, innov_ss, innov_rs,
    gather_ss, gather_rs, share_ss, share_rs, mem_ss, mem_rs, lat_ss, lat_rs, lon_ss, lon_rs, pair_ss, pair_rs,
):
    lat, lon, mem = lax.axis_index("lat"), lax.axis_index("lon"), lax.axis_index("mem")
    place_count = lat_size * lon_size
    half = lon_size // 2
    quarter = half // 2
    me = lat * lon_size + lon
    side = lax.div(lon, half)
    receives = lax.div(lax.rem(lon, half), quarter) == mem
    col_count, row_count = fields.shape[3:]
    f32, bf16 = jnp.float32, jnp.bfloat16

    def device(lat_idx, lon_idx, mem_idx):
        return {"lat": lat_idx, "lon": lon_idx, "mem": mem_idx}

    partner = device(lat, lon, 1 - mem)

    def remote(src, dst, send, recv, target):
        return pltpu.make_async_remote_copy(
            src_ref=src, dst_ref=dst, send_sem=send, recv_sem=recv,
            device_id=target, device_id_type=pl.DeviceIdType.MESH,
        )

    def owned(idx, core):
        near = lax.div(idx, quarter)
        return (1 - side + near * (2 * side - 1)) * half + core * quarter + lax.rem(idx, quarter)

    barrier = pltpu.get_barrier_semaphore()

    @pl.loop(1, place_count)
    def _(offset):
        spot = lax.rem(me + offset, place_count)
        pl.semaphore_signal(
            barrier, inc=1, device_id=device(lax.div(spot, lon_size), lax.rem(spot, lon_size), mem),
            device_id_type=pl.DeviceIdType.MESH,
        )

    pl.semaphore_signal(barrier, inc=1, device_id=partner, device_id_type=pl.DeviceIdType.MESH)
    pl.semaphore_wait(barrier, place_count)

    def field_copy(turn, slot, step):
        lat_idx, lon_idx = lax.rem(lat + slot, lat_size), lax.rem(lon + step, lon_size)
        return remote(
            anom.at[lat_idx * own + turn, lon_idx], fields.at[turn, slot, lon],
            field_ss.at[turn, slot, step], field_rs.at[turn, slot, step], device(lat_idx, lon_idx, mem),
        )

    def send_fields(turn, slot):
        @pl.loop(1 if slot == 0 else 0, lon_size)
        def _(step):
            field_copy(turn, slot, step).start()

    def own_copy(turn):
        return pltpu.make_async_copy(
            anom.at[lat * own + turn, lon], fields.at[turn, 0, lon], local_sem.at[turn]
        )

    lead = lat_size // 2
    for slot in range(lead):
        send_fields(0, slot)
    near_copies = [
        pltpu.make_async_copy(src, dst, table_sem.at[idx])
        for idx, (src, dst) in enumerate([
            (level, level_near), (column, column_near), (row, row_near), (value, value_near),
            (taper.at[0], taper_near), (coarse, coarse_near), (lon_high, high_near), (lon_low, low_near),
            (lat_high, lat_high_near), (lat_low, lat_low_near),
        ])
    ]
    for copy in near_copies:
        copy.start()
    for turn in range(own):
        own_copy(turn).start()

    hits[...] = jnp.zeros_like(hits)
    col_start, row_start = lon * col_count, lat * row_count
    group = 4
    for copy in near_copies[:4]:
        copy.wait()

    @pl.loop(0, obs_rows // group)
    def _(step):
        def wide(ref):
            return jnp.concatenate([ref[pl.ds(step * group + part, 1), :] for part in range(group)], axis=1)

        keys = wide(level_near) * col_count + (wide(column_near) - col_start)
        local_row = wide(row_near) - row_start
        amount = wide(value_near)
        width = keys.shape[1]
        high = amount.astype(bf16).astype(f32)
        low = amount - high
        row_hot = lax.broadcasted_iota(jnp.int32, (row_count, width), 0) == local_row
        right = jnp.concatenate(
            [jnp.where(row_hot, high, 0.0).astype(bf16), jnp.where(row_hot, low, 0.0).astype(bf16)], axis=0
        )
        cells = lax.broadcasted_iota(jnp.int32, (col_count, width), 0)
        for idx in range(half):
            left = jnp.where(cells == keys - owned(idx, mem) * col_count, 1.0, 0.0).astype(bf16)
            hits[idx] += lax.dot_general(
                left, right, (((1,), (1,)), ((), ())), preferred_element_type=f32
            )

    def innov_copy(idx):
        lev = owned(idx, mem)
        return remote(
            innov_own.at[idx], innov_all.at[0, lon], innov_ss.at[idx], innov_rs.at[lon], device(lat, lev, mem)
        )

    for idx in range(half):
        block = (hits[idx, :, :row_count] + hits[idx, :, row_count:]).astype(bf16)
        innov_own[idx] = block
        lev = owned(idx, mem)
        pl.when(lev != lon)(lambda idx=idx: innov_copy(idx).start())

        @pl.when(lev == lon)
        def _(block=block):
            innov_all[0, lon] = block

    for slot in range(lead, lat_size):
        send_fields(0, slot)
    near_copies[4].wait()
    taper_all[lat] = taper_near[...].astype(bf16)
    taper_copies = [
        remote(
            taper_all.at[lat], taper_all.at[lat], taper_ss.at[step], taper_rs.at[step],
            device(lax.rem(lat + step, lat_size), lon, mem),
        )
        for step in range(1, lat_size)
    ]
    for copy in taper_copies:
        copy.start()
    for copy in near_copies[5:]:
        copy.wait()

    outer, inner = high_near.shape[2], low_near.shape[2]

    @pl.loop(0, lat_size)
    def _(part):
        low_cos, low_sin = low_near[0, part], low_near[1, part]
        for idx in range(outer):
            high_cos, high_sin = high_near[0, part, idx:idx + 1, :], high_near[1, part, idx:idx + 1, :]
            rows = slice(idx * inner, (idx + 1) * inner)
            fine[0, rows, :] = high_cos * low_cos - high_sin * low_sin
            fine[1, rows, :] = high_sin * low_cos + high_cos * low_sin

        @pl.loop(0, lon_size)
        def _(block):
            table = (
                coarse_near[block, part, 0:1, :] * fine[0] + coarse_near[block, part, 1:2, :] * fine[1]
            )
            table_inv[block, part] = table.astype(bf16)
            table_fwd[block, part] = table.T.astype(bf16)

    lat_inner = lat_low_near.shape[1]
    per_band = row_count // lat_inner
    lat_cos, lat_sin = lat_low_near[0], lat_low_near[1]
    for slot in range(lat_size):
        band = lax.rem(lat + lat_size - slot, lat_size)
        for idx in range(per_band):
            spot = pl.ds(band * per_band + idx, 1)
            rows = slice(slot * row_count + idx * lat_inner, slot * row_count + (idx + 1) * lat_inner)
            modes[rows, :] = (
                lat_high_near[0, spot, :] * lat_cos - lat_high_near[1, spot, :] * lat_sin
            ).astype(bf16)

    def gather_copy(slot):
        return remote(
            innov_all.at[0], innov_all.at[slot], gather_ss.at[slot], gather_rs.at[slot],
            device(lax.rem(lat + slot, lat_size), lon, mem),
        )

    def share_copy(slot):
        return remote(innov_all.at[slot], innov_all.at[slot], share_ss.at[slot], share_rs.at[slot], partner)

    @pl.when(receives)
    def _():
        for step in range(1, lon_size):
            sender = lax.rem(lon + step, lon_size)
            remote(
                innov_own.at[0], innov_all.at[0, sender], innov_ss.at[0], innov_rs.at[sender],
                device(lat, sender, mem),
            ).wait_recv()
        for slot in range(1, lat_size):
            gather_copy(slot).start()
        share_copy(0).start()

    for turn in range(1, own):
        for slot in range(lat_size):
            send_fields(turn, slot)

    @pl.when(receives)
    def _():
        for slot in range(1, lat_size):
            gather_copy(slot).wait_recv()
            share_copy(slot).start()

    @pl.when(jnp.logical_not(receives))
    def _():
        for slot in range(lat_size):
            share_copy(slot).wait_recv()

    total[...] = jnp.zeros_like(total)
    for copy in taper_copies:
        copy.wait_recv()

    def transform(turn):
        def weigh(slot, block, lanes):
            weighted[block, :, lanes] = fields[turn, slot, block] * innov_all[slot, block]

        for stage in range(lat_size // 2):
            for which in range(2):
                slot = 2 * stage + which
                lanes = slice(which * row_count, (which + 1) * row_count)
                if slot == 0:
                    own_copy(turn).wait()
                    weigh(0, lon, lanes)

                @pl.loop(1 if slot == 0 else 0, lon_size)
                def _(step, slot=slot, lanes=lanes):
                    field_copy(turn, slot, step).wait_recv()
                    weigh(slot, lax.rem(lon + lon_size - step, lon_size), lanes)

            rows = slice(2 * stage * row_count, 2 * (stage + 1) * row_count)

            @pl.loop(0, lat_size)
            def _(part, stage=stage, rows=rows):
                zonal = jnp.dot(table_fwd[0, part], weighted[0], preferred_element_type=f32)
                for block in range(1, lon_size):
                    zonal += jnp.dot(table_fwd[block, part], weighted[block], preferred_element_type=f32)
                terms = jnp.dot(zonal.astype(bf16), modes[rows, :], preferred_element_type=f32)
                if stage > 0:
                    terms += spectrum[part]
                if stage < lat_size // 2 - 1:
                    spectrum[part] = terms
                else:
                    tapered = (terms * taper_all[part].astype(f32)).astype(bf16)
                    inverse[part] = lax.dot_general(
                        tapered, modes[...], (((1,), (1,)), ((), ())), preferred_element_type=f32
                    ).astype(bf16)

    def localize(turn, block):
        localized = jnp.dot(table_inv[block, 0], inverse[0], preferred_element_type=f32)
        for part in range(1, lat_size):
            localized += jnp.dot(table_inv[block, part], inverse[part], preferred_element_type=f32)
        for slot in range(lat_size):
            total[block, slot] += (
                fields[turn, slot, block].astype(f32)
                * localized[:, slot * row_count:(slot + 1) * row_count]
            )

    @pl.loop(0, own - 1)
    def _(turn):
        transform(turn)
        pl.loop(0, lon_size)(lambda block: localize(turn, block))

    transform(own - 1)

    def mem_copy(idx):
        return remote(
            total.at[owned(idx, 1 - mem)], partner_part.at[idx], mem_ss.at[idx], mem_rs.at[idx], partner
        )

    @pl.loop(0, half)
    def _(idx):
        localize(own - 1, owned(idx, 1 - mem))
        mem_copy(idx).start()

    def lat_copy(idx, slot):
        return remote(
            lat_send.at[idx, slot], lat_recv.at[idx, slot], lat_ss.at[idx, slot], lat_rs.at[idx, slot],
            device(lax.rem(lat + lat_size - slot, lat_size), lon, mem),
        )

    @pl.loop(0, half)
    def _(idx):
        block = owned(idx, mem)
        localize(own - 1, block)
        mem_copy(idx).wait_recv()
        for slot in list(range(1, lat_size)) + [0]:
            lat_send[idx, slot] = (total[block, slot] + partner_part[idx, slot]).astype(bf16)
            if slot > 0:
                lat_copy(idx, slot).start()

    def lon_copy(idx):
        return remote(
            lon_send.at[idx], lon_recv.at[lon], lon_ss.at[idx], lon_rs.at[lon], device(lat, owned(idx, mem), mem)
        )

    for idx in range(half):
        summed = lat_send[idx, 0].astype(f32)
        for slot in range(1, lat_size):
            lat_copy(idx, slot).wait_recv()
            summed += lat_recv[idx, slot].astype(f32)
        block = owned(idx, mem)
        lon_send[idx] = summed.astype(bf16)
        pl.when(block != lon)(lambda idx=idx: lon_copy(idx).start())

        @pl.when(block == lon)
        def _(idx=idx):
            lon_recv[lon] = lon_send[idx]

    def pair_copy(sender):
        return remote(lon_recv.at[sender], lon_recv.at[sender], pair_ss.at[sender], pair_rs.at[sender], partner)

    far = [(1 - side) * half + idx for idx in range(half)]
    close = [side * half + lax.rem(lon + idx, half) for idx in range(1, half)]

    @pl.when(receives)
    def _():
        pair_copy(lon).start()
        for sender in far + close:
            remote(
                lon_send.at[0], lon_recv.at[sender], lon_ss.at[0], lon_rs.at[sender], device(lat, sender, mem)
            ).wait_recv()
            pair_copy(sender).start()

    @pl.when(jnp.logical_not(receives))
    def _():
        for sender in far + close + [lon]:
            pair_copy(sender).wait_recv()

    out[...] = lon_recv[...]

    @pl.when(receives)
    def _():
        for sender in far + close + [lon]:
            pair_copy(sender).wait_send()
        for slot in range(1, lat_size):
            gather_copy(slot).wait_send()
        for slot in range(lat_size):
            share_copy(slot).wait_send()

    for idx in range(half):
        pl.when(owned(idx, mem) != lon)(lambda idx=idx: lon_copy(idx).wait_send())
        pl.when(owned(idx, mem) != lon)(lambda idx=idx: innov_copy(idx).wait_send())
        mem_copy(idx).wait_send()
        for slot in range(1, lat_size):
            lat_copy(idx, slot).wait_send()
    for copy in taper_copies:
        copy.wait_send()

    @pl.loop(0, own)
    def _(turn):
        for slot in range(lat_size):
            @pl.loop(1 if slot == 0 else 0, lon_size)
            def _(step, slot=slot):
                field_copy(turn, slot, step).wait_send()


def local(anomalies, taper, obs_row, obs_col, obs_level, obs_value):
    member_count, level_count, col_count, row_count = anomalies.shape
    lon_size, lat_size = lax.axis_size("lon"), lax.axis_size("lat")
    lat_total = row_count * lat_size
    ensemble = member_count * lax.axis_size("mem")
    own = member_count // lat_size
    half = lon_size // 2
    part_count = taper.shape[1]
    seeds = lon_seeds(lon_size, col_count, lat_size, part_count) + lat_seeds(lat_total)
    f32, bf16 = jnp.float32, jnp.bfloat16
    slab = (col_count, row_count)
    whole = pl.BlockSpec(memory_space=pl.ANY)
    dma = pltpu.SemaphoreType.DMA
    obs = [(table.shape, table.dtype) for table in (obs_level, obs_col, obs_row, obs_value)]
    near = obs + [(seed.shape, f32) for seed in seeds]
    result = pl.pallas_call(
        functools.partial(fused_kernel, lat_size, lon_size, own, obs_row.shape[0]),
        out_shape=jax.ShapeDtypeStruct((level_count,) + slab, bf16),
        in_specs=[whole] * 11,
        out_specs=pl.BlockSpec(memory_space=pltpu.VMEM),
        scratch_shapes=[
            pltpu.VMEM((own, lat_size, lon_size) + slab, bf16),
            pltpu.VMEM((lon_size, lat_size, part_count, col_count), bf16),
            pltpu.VMEM((lon_size, lat_size, col_count, part_count), bf16),
            pltpu.VMEM((2, col_count, part_count), f32),
            pltpu.VMEM((lat_total, lat_total), bf16),
            pltpu.VMEM((part_count, lat_total), f32),
            pltpu.VMEM((lat_size, part_count, lat_total), bf16),
            pltpu.VMEM((half, col_count, 2 * row_count), f32),
            pltpu.VMEM((half,) + slab, bf16),
            pltpu.VMEM((lat_size, lon_size) + slab, bf16),
            pltpu.VMEM((lon_size, col_count, 2 * row_count), bf16),
            pltpu.VMEM((lat_size, part_count, lat_total), f32),
            pltpu.VMEM((lat_size, part_count, lat_total), bf16),
            pltpu.VMEM((lon_size, lat_size) + slab, f32),
            pltpu.VMEM((half, lat_size) + slab, f32),
            pltpu.VMEM((half, lat_size) + slab, bf16),
            pltpu.VMEM((half, lat_size) + slab, bf16),
            pltpu.VMEM((half,) + slab, bf16),
            pltpu.VMEM((level_count,) + slab, bf16),
            *[pltpu.VMEM(shape, dtype) for shape, dtype in near],
            dma((own, lat_size, lon_size)), dma((own, lat_size, lon_size)), dma((own,)), dma((10,)),
            dma((lat_size,)), dma((lat_size,)), dma((half,)), dma((lon_size,)),
            dma((lat_size,)), dma((lat_size,)), dma((lat_size,)), dma((lat_size,)),
            dma((half,)), dma((half,)), dma((half, lat_size)), dma((half, lat_size)),
            dma((half,)), dma((lon_size,)), dma((lon_size,)), dma((lon_size,)),
        ],
        compiler_params=pltpu.CompilerParams(
            collective_id=0, has_side_effects=True, vmem_limit_bytes=60 * 1024 * 1024
        ),
    )(
        anomalies, taper, obs_level, obs_col, obs_row, obs_value, *seeds,
    )
    return result.astype(f32) / (ensemble - 1)


def solution(mesh):
    in_specs = (
        P("mem", None, "lon", "lat"),
        P("lon", "lat", None),
        P("lat", "lon"),
        P("lat", "lon"),
        P("lat", "lon"),
        P("lat", "lon"),
    )
    out_specs = P(None, "lon", "lat")
    return jax.shard_map(local, mesh=mesh, in_specs=in_specs, out_specs=out_specs, check_vma=False)
```

```python
import functools
import math

import jax
import jax.numpy as jnp
import numpy as np
from jax import lax
from jax.experimental import pallas as pl
from jax.experimental.pallas import tpu as pltpu
from jax.sharding import PartitionSpec as P


CLASSES = (0, 2, 1, 3)


def round_up(size, unit):
    return -(-size // unit) * unit


def lon_seeds(length, part_count):
    nyquist = length // 2
    quarter = length // 4
    inner = next(n for n in range(24, 0, -8) if quarter % n == 0)
    outer = quarter // inner
    share = quarter // part_count
    padded = round_up(share, 16)
    offsets = np.arange(padded)
    coef_idx = np.stack([
        np.stack([part * (length // part_count) + 4 * offsets + kind for part in range(part_count)])
        for kind in CLASSES
    ])
    real = np.broadcast_to(offsets < share, coef_idx.shape).reshape(-1)
    coef_idx = np.where(real, coef_idx.reshape(-1), 0)
    wavenum = np.where(coef_idx <= nyquist, coef_idx, coef_idx - nyquist)

    def waves(points):
        angles = (points[:, None] * wavenum[None, :] % length) * (2.0 * math.pi / length)
        return np.cos(angles), np.sin(angles)

    scales = np.where((coef_idx == 0) | (coef_idx == nyquist), 1.0 / math.sqrt(length), math.sqrt(2.0 / length))
    scales = np.where(real, scales, 0.0)
    is_cos = coef_idx <= nyquist
    starts = np.arange(2)[:, None] * quarter + np.arange(outer)[None, :] * inner
    high_cos, high_sin = waves(starts.reshape(-1))
    first = np.where(is_cos, high_cos, high_sin) * scales
    second = np.where(is_cos, -high_sin, high_cos) * scales
    high = np.stack([first, second]).reshape(2, 2, outer, -1)
    low = np.stack(waves(np.arange(inner)))
    return [jnp.asarray(part, jnp.float32) for part in (high, low)]


def lat_seeds(length):
    inner = next(size for size in range(32, 0, -1) if length % size == 0)
    outer = length // inner
    mode_idx = np.arange(length)[None, :]

    def waves(points):
        angles = (mode_idx * points[:, None] % (4 * length)) * (math.pi / (2.0 * length))
        return np.cos(angles), np.sin(angles)

    scales = np.where(mode_idx == 0, 1.0 / math.sqrt(length), math.sqrt(2.0 / length))
    high = np.stack(waves(np.arange(outer) * (2 * inner))) * scales
    low = np.stack(waves(np.arange(inner) * 2 + 1))
    return [jnp.asarray(part, jnp.float32) for part in (high, low)]


def fused_kernel(
    lat_size, lon_size, own, obs_rows,
    anom, taper, level, column, row, value, lon_high, lon_low, lat_high, lat_low, out,
    fields, even_fwd, odd_fwd, even_inv, odd_inv, fine, modes, taper_near, taper_all, hits, innov_own, innov_all,
    folded, zonal, spectrum, tapered, inverse, total, partner_part, lat_send, lat_recv, lon_send, lon_recv,
    level_near, column_near, row_near, value_near, high_near, low_near, lat_high_near, lat_low_near,
    field_ss, field_rs, local_sem, table_sem, taper_ss, taper_rs, trade_ss, trade_rs, innov_ss, innov_rs,
    gather_ss, gather_rs, share_ss, share_rs, mem_ss, mem_rs, lat_ss, lat_rs, lon_ss, lon_rs, pair_ss, pair_rs,
):
    lat, lon, mem = lax.axis_index("lat"), lax.axis_index("lon"), lax.axis_index("mem")
    place_count = lat_size * lon_size
    half = lon_size // 2
    quarter = half // 2
    me = lat * lon_size + lon
    side = lax.div(lon, half)
    receives = lax.div(lax.rem(lon, half), quarter) == mem
    col_count, row_count = fields.shape[3:]
    f32, bf16 = jnp.float32, jnp.bfloat16

    def device(lat_idx, lon_idx, mem_idx):
        return {"lat": lat_idx, "lon": lon_idx, "mem": mem_idx}

    partner = device(lat, lon, 1 - mem)

    def remote(src, dst, send, recv, target):
        return pltpu.make_async_remote_copy(
            src_ref=src, dst_ref=dst, send_sem=send, recv_sem=recv,
            device_id=target, device_id_type=pl.DeviceIdType.MESH,
        )

    def owned(idx, core):
        near = lax.div(idx, quarter)
        return (1 - side + near * (2 * side - 1)) * half + core * quarter + lax.rem(idx, quarter)

    barrier = pltpu.get_barrier_semaphore()

    @pl.loop(1, place_count)
    def _(offset):
        spot = lax.rem(me + offset, place_count)
        pl.semaphore_signal(
            barrier, inc=1, device_id=device(lax.div(spot, lon_size), lax.rem(spot, lon_size), mem),
            device_id_type=pl.DeviceIdType.MESH,
        )

    pl.semaphore_signal(barrier, inc=1, device_id=partner, device_id_type=pl.DeviceIdType.MESH)
    pl.semaphore_wait(barrier, place_count)

    def field_copy(turn, slot, step):
        lat_idx, lon_idx = lax.rem(lat + slot, lat_size), lax.rem(lon + step, lon_size)
        return remote(
            anom.at[lat_idx * own + turn, lon_idx], fields.at[turn, slot, lon],
            field_ss.at[turn, slot, step], field_rs.at[turn, slot, step], device(lat_idx, lon_idx, mem),
        )

    def send_fields(turn, slot):
        @pl.loop(1 if slot == 0 else 0, lon_size)
        def _(step):
            field_copy(turn, slot, step).start()

    def own_copy(turn):
        return pltpu.make_async_copy(
            anom.at[lat * own + turn, lon], fields.at[turn, 0, lon], local_sem.at[turn]
        )

    lead = lat_size // 2
    for slot in range(lead):
        send_fields(0, slot)
    near_copies = [
        pltpu.make_async_copy(src, dst, table_sem.at[idx])
        for idx, (src, dst) in enumerate([
            (level, level_near), (column, column_near), (row, row_near), (value, value_near),
            (taper.at[0], taper_near), (lon_high, high_near), (lon_low, low_near),
            (lat_high, lat_high_near), (lat_low, lat_low_near),
        ])
    ]
    for copy in near_copies:
        copy.start()
    for turn in range(own):
        own_copy(turn).start()

    hits[...] = jnp.zeros_like(hits)
    col_start, row_start = lon * col_count, lat * row_count
    group = 4
    for copy in near_copies[:4]:
        copy.wait()

    @pl.loop(0, obs_rows // group)
    def _(step):
        def wide(ref):
            return jnp.concatenate([ref[pl.ds(step * group + part, 1), :] for part in range(group)], axis=1)

        keys = wide(level_near) * col_count + (wide(column_near) - col_start)
        local_row = wide(row_near) - row_start
        amount = wide(value_near)
        width = keys.shape[1]
        high = amount.astype(bf16).astype(f32)
        low = amount - high
        row_hot = lax.broadcasted_iota(jnp.int32, (row_count, width), 0) == local_row
        right = jnp.concatenate(
            [jnp.where(row_hot, high, 0.0).astype(bf16), jnp.where(row_hot, low, 0.0).astype(bf16)], axis=0
        )
        cells = lax.broadcasted_iota(jnp.int32, (col_count, width), 0)
        for idx in range(half):
            left = jnp.where(cells == keys - owned(idx, mem) * col_count, 1.0, 0.0).astype(bf16)
            hits[idx] += lax.dot_general(
                left, right, (((1,), (1,)), ((), ())), preferred_element_type=f32
            )

    def innov_copy(idx):
        lev = owned(idx, mem)
        return remote(
            innov_own.at[idx], innov_all.at[0, lon], innov_ss.at[idx], innov_rs.at[lon], device(lat, lev, mem)
        )

    for idx in range(half):
        block = (hits[idx, :, :row_count] + hits[idx, :, row_count:]).astype(bf16)
        innov_own[idx] = block
        lev = owned(idx, mem)
        pl.when(lev != lon)(lambda idx=idx: innov_copy(idx).start())

        @pl.when(lev == lon)
        def _(block=block):
            innov_all[0, lon] = block

    for slot in range(lead, lat_size):
        send_fields(0, slot)
    near_copies[4].wait()
    share, share_pad = taper_near.shape[0] // 4, taper_all.shape[2]
    modes_half = taper_near.shape[1] // 2
    spread = (4 * share_pad, 4 * share)
    out_row = lax.broadcasted_iota(jnp.int32, spread, 0)
    in_row = lax.broadcasted_iota(jnp.int32, spread, 1)
    chosen = jnp.zeros(spread, jnp.bool_)
    for idx, kind in enumerate(CLASSES):
        local_row = out_row - idx * share_pad
        chosen |= (local_row >= 0) & (local_row < share) & (in_row == 4 * local_row + kind)
    by_class = jnp.dot(
        jnp.where(chosen, 1.0, 0.0).astype(bf16), taper_near[...].astype(bf16), preferred_element_type=f32
    ).astype(bf16)
    for idx in range(4):
        taper_all[idx, lat] = by_class[idx * share_pad:(idx + 1) * share_pad]
    lanes = pl.ds(pl.multiple_of(mem * modes_half, modes_half), modes_half)

    def taper_copy(step):
        part = taper_all.at[:, lat, :, lanes]
        return remote(
            part, part, taper_ss.at[step], taper_rs.at[step], device(lax.rem(lat + step, lat_size), lon, mem)
        )

    def trade_copy(step):
        part = taper_all.at[:, lax.rem(lat + lat_size - step, lat_size), :, lanes]
        return remote(part, part, trade_ss.at[step], trade_rs.at[step], partner)

    for step in range(1, lat_size):
        taper_copy(step).start()
    for copy in near_copies[5:]:
        copy.wait()

    outer, inner = high_near.shape[2], low_near.shape[1]
    points, kind_size = even_inv.shape[1:]
    span = outer * inner
    low_cos, low_sin = low_near[0], low_near[1]
    fine[span:, :] = jnp.zeros((points - span, 4 * kind_size), f32)
    for block in range(2):
        first = 2 * block * kind_size
        for idx in range(outer):
            fine[idx * inner:(idx + 1) * inner, first:] = (
                high_near[0, block, idx:idx + 1, first:] * low_cos[:, first:]
                + high_near[1, block, idx:idx + 1, first:] * low_sin[:, first:]
            )
        for kind in range(2 * block, 4):
            tile = fine[:, kind * kind_size:(kind + 1) * kind_size]
            if kind < 2:
                even_inv[kind] = tile.astype(bf16)
                even_fwd[kind] = tile.T.astype(bf16)
            else:
                rows = slice(block * points, (block + 1) * points)
                cols = slice((kind - 2) * kind_size, (kind - 1) * kind_size)
                odd_inv[rows, cols] = tile.astype(bf16)
                odd_fwd[cols, rows] = tile.T.astype(bf16)
    folded[...] = jnp.zeros_like(folded)

    lat_inner = lat_low_near.shape[1]
    per_band = row_count // lat_inner
    lat_cos, lat_sin = lat_low_near[0], lat_low_near[1]
    for slot in range(lat_size):
        band = lax.rem(lat + lat_size - slot, lat_size)
        for idx in range(per_band):
            spot = pl.ds(band * per_band + idx, 1)
            rows = slice(slot * row_count + idx * lat_inner, slot * row_count + (idx + 1) * lat_inner)
            modes[rows, :] = (
                lat_high_near[0, spot, :] * lat_cos - lat_high_near[1, spot, :] * lat_sin
            ).astype(bf16)

    def gather_copy(slot):
        return remote(
            innov_all.at[0], innov_all.at[slot], gather_ss.at[slot], gather_rs.at[slot],
            device(lax.rem(lat + slot, lat_size), lon, mem),
        )

    def share_copy(slot):
        return remote(innov_all.at[slot], innov_all.at[slot], share_ss.at[slot], share_rs.at[slot], partner)

    @pl.when(receives)
    def _():
        for step in range(1, lon_size):
            sender = lax.rem(lon + step, lon_size)
            remote(
                innov_own.at[0], innov_all.at[0, sender], innov_ss.at[0], innov_rs.at[sender],
                device(lat, sender, mem),
            ).wait_recv()
        for slot in range(1, lat_size):
            gather_copy(slot).start()
        share_copy(0).start()

    for turn in range(1, own):
        for slot in range(lat_size):
            send_fields(turn, slot)

    @pl.when(receives)
    def _():
        for slot in range(1, lat_size):
            gather_copy(slot).wait_recv()
            share_copy(slot).start()

    @pl.when(jnp.logical_not(receives))
    def _():
        for slot in range(lat_size):
            share_copy(slot).wait_recv()

    total[...] = jnp.zeros_like(total)
    for step in range(1, lat_size):
        taper_copy(step).wait_recv()
        trade_copy(step).start()
    for step in range(1, lat_size):
        trade_copy(step).wait_recv()

    stages = lat_size // 2
    pair = 2 * row_count
    fourth = lon_size // 4
    kinds = 4 * kind_size

    def fold(turn, slot, lanes):
        def quarter_of(which):
            parts = []
            for idx in range(fourth):
                block = which * fourth + idx
                parts.append(fields[turn, slot, block].astype(f32) * innov_all[slot, block].astype(f32))
            return parts[0] if fourth == 1 else jnp.concatenate(parts, axis=0)

        first, second, third, last = [quarter_of(which) for which in range(4)]
        even, odd = first + third, second + last
        for idx, value in enumerate([even + odd, even - odd, first - third, second - last]):
            folded[pl.ds(idx * points, span), lanes] = value.astype(bf16)

    def transform(turn):
        @pl.loop(0, stages)
        def _(stage):
            for which in range(2):
                slot = 2 * stage + which

                @pl.loop(0, lon_size)
                def _(step, slot=slot):
                    pl.when(slot + step == 0)(lambda: own_copy(turn).wait())
                    pl.when(slot + step > 0)(lambda: field_copy(turn, slot, step).wait_recv())

                fold(turn, slot, slice(which * row_count, (which + 1) * row_count))
            for kind in range(2):
                zonal[kind * kind_size:(kind + 1) * kind_size, :] = jnp.dot(
                    even_fwd[kind], folded[kind * points:(kind + 1) * points, :], preferred_element_type=f32
                ).astype(bf16)
            zonal[2 * kind_size:, :] = jnp.dot(
                odd_fwd[...], folded[2 * points:, :], preferred_element_type=f32
            ).astype(bf16)
            terms = jnp.dot(
                zonal[...], modes[pl.ds(pl.multiple_of(stage * pair, pair), pair), :], preferred_element_type=f32
            )

            @pl.when(stage == 0)
            def _():
                spectrum[...] = terms

            @pl.when(stage > 0)
            def _():
                spectrum[...] += terms

        tapered[...] = (
            spectrum[...] * taper_all[...].reshape(kinds, lat_size * row_count).astype(f32)
        ).astype(bf16)
        inverse[...] = lax.dot_general(
            tapered[...], modes[...], (((1,), (1,)), ((), ())), preferred_element_type=f32
        ).astype(bf16)

    def localize(turn, stage):
        lanes = pl.ds(pl.multiple_of(stage * pair, pair), pair)

        def back(table, rows):
            return jnp.dot(table, inverse[rows, lanes], preferred_element_type=f32)

        even = back(even_inv[0, :span], slice(0, kind_size))
        swing = back(even_inv[1, :span], slice(kind_size, 2 * kind_size))
        odd = [back(odd_inv[idx * points:idx * points + span, :], slice(2 * kind_size, kinds)) for idx in range(2)]
        for which in range(4):
            base = even + swing if which % 2 == 0 else even - swing
            values = base + odd[which % 2] if which < 2 else base - odd[which % 2]
            for idx in range(fourth):
                block = which * fourth + idx
                for part in range(2):
                    slot = 2 * stage + part
                    total[block, slot] += (
                        fields[turn, slot, block].astype(f32)
                        * values[idx * col_count:(idx + 1) * col_count, part * row_count:(part + 1) * row_count]
                    )

    @pl.loop(0, own - 1)
    def _(turn):
        transform(turn)
        pl.loop(0, stages)(lambda stage: localize(turn, stage))

    transform(own - 1)

    def mem_copy(idx, stage):
        slots = pl.ds(2 * stage, 2)
        return remote(
            total.at[owned(idx, 1 - mem), slots], partner_part.at[idx, slots],
            mem_ss.at[idx, stage], mem_rs.at[idx, stage], partner,
        )

    @pl.loop(0, stages)
    def _(step):
        stage = stages - 1 - step
        localize(own - 1, stage)
        for idx in range(half):
            mem_copy(idx, stage).start()

    def lat_copy(idx, slot):
        return remote(
            lat_send.at[idx, slot], lat_recv.at[idx, slot], lat_ss.at[idx, slot], lat_rs.at[idx, slot],
            device(lax.rem(lat + lat_size - slot, lat_size), lon, mem),
        )

    @pl.loop(0, half)
    def _(idx):
        block = owned(idx, mem)
        for stage in range(stages - 1, -1, -1):
            mem_copy(idx, stage).wait_recv()
            for slot in (2 * stage + 1, 2 * stage):
                lat_send[idx, slot] = (total[block, slot] + partner_part[idx, slot]).astype(bf16)
                if slot > 0:
                    lat_copy(idx, slot).start()

    def lon_copy(idx):
        return remote(
            lon_send.at[idx], lon_recv.at[lon], lon_ss.at[idx], lon_rs.at[lon], device(lat, owned(idx, mem), mem)
        )

    for idx in range(half):
        summed = lat_send[idx, 0].astype(f32)
        for slot in range(1, lat_size):
            lat_copy(idx, slot).wait_recv()
            summed += lat_recv[idx, slot].astype(f32)
        block = owned(idx, mem)
        lon_send[idx] = summed.astype(bf16)
        pl.when(block != lon)(lambda idx=idx: lon_copy(idx).start())

        @pl.when(block == lon)
        def _(idx=idx):
            lon_recv[lon] = lon_send[idx]

    def pair_copy(sender):
        return remote(lon_recv.at[sender], lon_recv.at[sender], pair_ss.at[sender], pair_rs.at[sender], partner)

    far = [(1 - side) * half + idx for idx in range(half)]
    close = [side * half + lax.rem(lon + idx, half) for idx in range(1, half)]

    @pl.when(receives)
    def _():
        pair_copy(lon).start()
        for sender in far + close:
            remote(
                lon_send.at[0], lon_recv.at[sender], lon_ss.at[0], lon_rs.at[sender], device(lat, sender, mem)
            ).wait_recv()
            pair_copy(sender).start()

    @pl.when(jnp.logical_not(receives))
    def _():
        for sender in far + close + [lon]:
            pair_copy(sender).wait_recv()

    out[...] = lon_recv[...]

    @pl.when(receives)
    def _():
        for sender in far + close + [lon]:
            pair_copy(sender).wait_send()
        for slot in range(1, lat_size):
            gather_copy(slot).wait_send()
        for slot in range(lat_size):
            share_copy(slot).wait_send()

    for idx in range(half):
        pl.when(owned(idx, mem) != lon)(lambda idx=idx: lon_copy(idx).wait_send())
        pl.when(owned(idx, mem) != lon)(lambda idx=idx: innov_copy(idx).wait_send())
        for stage in range(stages):
            mem_copy(idx, stage).wait_send()
        for slot in range(1, lat_size):
            lat_copy(idx, slot).wait_send()
    for step in range(1, lat_size):
        taper_copy(step).wait_send()
        trade_copy(step).wait_send()

    @pl.loop(0, own)
    def _(turn):
        for slot in range(lat_size):
            @pl.loop(1 if slot == 0 else 0, lon_size)
            def _(step, slot=slot):
                field_copy(turn, slot, step).wait_send()


def local(anomalies, taper, obs_row, obs_col, obs_level, obs_value):
    member_count, level_count, col_count, row_count = anomalies.shape
    lon_size, lat_size = lax.axis_size("lon"), lax.axis_size("lat")
    lat_total = row_count * lat_size
    ensemble = member_count * lax.axis_size("mem")
    own = member_count // lat_size
    half = lon_size // 2
    part_count = taper.shape[1]
    lon_total = col_count * lon_size
    seeds = lon_seeds(lon_total, lat_size) + lat_seeds(lat_total)
    share_pad = round_up(part_count // 4, 16)
    kind_size, points = lat_size * share_pad, round_up(lon_total // 4, 128)
    f32, bf16 = jnp.float32, jnp.bfloat16
    slab = (col_count, row_count)
    whole = pl.BlockSpec(memory_space=pl.ANY)
    dma = pltpu.SemaphoreType.DMA
    obs = [(table.shape, table.dtype) for table in (obs_level, obs_col, obs_row, obs_value)]
    near = obs + [(seed.shape, f32) for seed in seeds]
    result = pl.pallas_call(
        functools.partial(fused_kernel, lat_size, lon_size, own, obs_row.shape[0]),
        out_shape=jax.ShapeDtypeStruct((level_count,) + slab, bf16),
        in_specs=[whole] * 10,
        out_specs=pl.BlockSpec(memory_space=pltpu.VMEM),
        scratch_shapes=[
            pltpu.VMEM((own, lat_size, lon_size) + slab, bf16),
            pltpu.VMEM((2, kind_size, points), bf16),
            pltpu.VMEM((2 * kind_size, 2 * points), bf16),
            pltpu.VMEM((2, points, kind_size), bf16),
            pltpu.VMEM((2 * points, 2 * kind_size), bf16),
            pltpu.VMEM((points, 4 * kind_size), f32),
            pltpu.VMEM((lat_total, lat_total), bf16),
            pltpu.VMEM((part_count, lat_total), f32),
            pltpu.VMEM((4, lat_size, share_pad, lat_total), bf16),
            pltpu.VMEM((half, col_count, 2 * row_count), f32),
            pltpu.VMEM((half,) + slab, bf16),
            pltpu.VMEM((lat_size, lon_size) + slab, bf16),
            pltpu.VMEM((4 * points, 2 * row_count), bf16),
            pltpu.VMEM((4 * kind_size, 2 * row_count), bf16),
            pltpu.VMEM((4 * kind_size, lat_total), f32),
            pltpu.VMEM((4 * kind_size, lat_total), bf16),
            pltpu.VMEM((4 * kind_size, lat_total), bf16),
            pltpu.VMEM((lon_size, lat_size) + slab, f32),
            pltpu.VMEM((half, lat_size) + slab, f32),
            pltpu.VMEM((half, lat_size) + slab, bf16),
            pltpu.VMEM((half, lat_size) + slab, bf16),
            pltpu.VMEM((half,) + slab, bf16),
            pltpu.VMEM((level_count,) + slab, bf16),
            *[pltpu.VMEM(shape, dtype) for shape, dtype in near],
            dma((own, lat_size, lon_size)), dma((own, lat_size, lon_size)), dma((own,)), dma((9,)),
            dma((lat_size,)), dma((lat_size,)), dma((lat_size,)), dma((lat_size,)), dma((half,)), dma((lon_size,)),
            dma((lat_size,)), dma((lat_size,)), dma((lat_size,)), dma((lat_size,)),
            dma((half, lat_size // 2)), dma((half, lat_size // 2)), dma((half, lat_size)), dma((half, lat_size)),
            dma((half,)), dma((lon_size,)), dma((lon_size,)), dma((lon_size,)),
        ],
        compiler_params=pltpu.CompilerParams(
            collective_id=0, has_side_effects=True, vmem_limit_bytes=60 * 1024 * 1024
        ),
    )(
        anomalies, taper, obs_level, obs_col, obs_row, obs_value, *seeds,
    )
    return result.astype(f32) / (ensemble - 1)


def solution(mesh):
    in_specs = (
        P("mem", None, "lon", "lat"),
        P("lon", "lat", None),
        P("lat", "lon"),
        P("lat", "lon"),
        P("lat", "lon"),
        P("lat", "lon"),
    )
    out_specs = P(None, "lon", "lat")
    return jax.shard_map(local, mesh=mesh, in_specs=in_specs, out_specs=out_specs, check_vma=False)
```

```python
import functools
import math

import jax
import jax.numpy as jnp
import numpy as np
from jax import lax
from jax.experimental import pallas as pl
from jax.experimental.pallas import tpu as pltpu
from jax.sharding import PartitionSpec as P


CLASSES = (0, 2, 1, 3)


def round_up(size, unit):
    return -(-size // unit) * unit


def lon_seeds(length, part_count):
    nyquist = length // 2
    quarter = length // 4
    inner = next(n for n in range(24, 0, -8) if quarter % n == 0)
    outer = quarter // inner
    share = quarter // part_count
    padded = round_up(share, 16)
    offsets = np.arange(padded)
    coef_idx = np.stack([
        np.stack([part * (length // part_count) + 4 * offsets + kind for part in range(part_count)])
        for kind in CLASSES
    ])
    real = np.broadcast_to(offsets < share, coef_idx.shape).reshape(-1)
    coef_idx = np.where(real, coef_idx.reshape(-1), 0)
    wavenum = np.where(coef_idx <= nyquist, coef_idx, coef_idx - nyquist)

    def waves(points):
        angles = (points[:, None] * wavenum[None, :] % length) * (2.0 * math.pi / length)
        return np.cos(angles), np.sin(angles)

    scales = np.where((coef_idx == 0) | (coef_idx == nyquist), 1.0 / math.sqrt(length), math.sqrt(2.0 / length))
    scales = np.where(real, scales, 0.0)
    is_cos = coef_idx <= nyquist
    starts = np.arange(2)[:, None] * quarter + np.arange(outer)[None, :] * inner
    high_cos, high_sin = waves(starts.reshape(-1))
    first = np.where(is_cos, high_cos, high_sin) * scales
    second = np.where(is_cos, -high_sin, high_cos) * scales
    high = np.stack([first, second]).reshape(2, 2, outer, -1)
    low = np.stack(waves(np.arange(inner)))
    return [jnp.asarray(part, jnp.float32) for part in (high, low)]


def lat_seeds(length):
    inner = next(size for size in range(32, 0, -1) if length % size == 0)
    outer = length // inner
    mode_idx = np.arange(length)[None, :]

    def waves(points):
        angles = (mode_idx * points[:, None] % (4 * length)) * (math.pi / (2.0 * length))
        return np.cos(angles), np.sin(angles)

    scales = np.where(mode_idx == 0, 1.0 / math.sqrt(length), math.sqrt(2.0 / length))
    high = np.stack(waves(np.arange(outer) * (2 * inner))) * scales
    low = np.stack(waves(np.arange(inner) * 2 + 1))
    return [jnp.asarray(part, jnp.float32) for part in (high, low)]


def fused_kernel(
    lat_size, lon_size, own, obs_rows,
    anom, taper, level, column, row, value, lon_high, lon_low, lat_high, lat_low, out,
    fields, even_fwd, odd_fwd, even_inv, odd_inv, fine, modes, taper_near, taper_all, hits, innov_own, innov_all,
    folded, zonal, spectrum, tapered, inverse, total, partner_part, lat_send, lat_recv, near_send, near_recv, lon_send, lon_recv,
    level_near, column_near, row_near, value_near, high_near, low_near, lat_high_near, lat_low_near,
    field_ss, field_rs, local_sem, table_sem, taper_ss, taper_rs, trade_ss, trade_rs, innov_ss, innov_rs,
    gather_ss, gather_rs, share_ss, share_rs, mem_ss, mem_rs, lat_ss, lat_rs, near_ss, near_rs, lon_ss, lon_rs, pair_ss, pair_rs, out_sem,
):
    lat, lon, mem = lax.axis_index("lat"), lax.axis_index("lon"), lax.axis_index("mem")
    place_count = lat_size * lon_size
    half = lon_size // 2
    quarter = half // 2
    me = lat * lon_size + lon
    side = lax.div(lon, half)
    receives = lax.div(lax.rem(lon, half), quarter) == mem
    col_count, row_count = fields.shape[3:]
    f32, bf16 = jnp.float32, jnp.bfloat16

    def device(lat_idx, lon_idx, mem_idx):
        return {"lat": lat_idx, "lon": lon_idx, "mem": mem_idx}

    partner = device(lat, lon, 1 - mem)

    def remote(src, dst, send, recv, target):
        return pltpu.make_async_remote_copy(
            src_ref=src, dst_ref=dst, send_sem=send, recv_sem=recv,
            device_id=target, device_id_type=pl.DeviceIdType.MESH,
        )

    def owned(idx, core):
        near = lax.div(idx, quarter)
        return (1 - side + near * (2 * side - 1)) * half + core * quarter + lax.rem(idx, quarter)

    barrier = pltpu.get_barrier_semaphore()

    @pl.loop(1, place_count)
    def _(offset):
        spot = lax.rem(me + offset, place_count)
        pl.semaphore_signal(
            barrier, inc=1, device_id=device(lax.div(spot, lon_size), lax.rem(spot, lon_size), mem),
            device_id_type=pl.DeviceIdType.MESH,
        )

    pl.semaphore_signal(barrier, inc=1, device_id=partner, device_id_type=pl.DeviceIdType.MESH)
    pl.semaphore_wait(barrier, place_count)

    def field_copy(turn, slot, step):
        lat_idx, lon_idx = lax.rem(lat + slot, lat_size), lax.rem(lon + step, lon_size)
        return remote(
            anom.at[lat_idx * own + turn, lon_idx], fields.at[turn, slot, lon],
            field_ss.at[turn, slot, step], field_rs.at[turn, slot, step], device(lat_idx, lon_idx, mem),
        )

    def send_fields(turn, slot):
        @pl.loop(0, lon_size - 1 if slot == 0 else lon_size)
        def _(idx):
            step = half + lax.div(idx + 1, 2) * (1 - 2 * lax.rem(idx, 2))
            field_copy(turn, slot, step).start()

    def own_copy(turn):
        return pltpu.make_async_copy(
            anom.at[lat * own + turn, lon], fields.at[turn, 0, lon], local_sem.at[turn]
        )

    lead = lat_size // 2
    for slot in range(lead):
        send_fields(0, slot)
    near_copies = [
        pltpu.make_async_copy(src, dst, table_sem.at[idx])
        for idx, (src, dst) in enumerate([
            (level, level_near), (column, column_near), (row, row_near), (value, value_near),
            (taper.at[0], taper_near), (lon_high, high_near), (lon_low, low_near),
            (lat_high, lat_high_near), (lat_low, lat_low_near),
        ])
    ]
    for copy in near_copies:
        copy.start()
    for turn in range(own):
        own_copy(turn).start()

    hits[...] = jnp.zeros_like(hits)
    col_start, row_start = lon * col_count, lat * row_count
    group = 4
    for copy in near_copies[:4]:
        copy.wait()

    @pl.loop(0, obs_rows // group)
    def _(step):
        def wide(ref):
            return jnp.concatenate([ref[pl.ds(step * group + part, 1), :] for part in range(group)], axis=1)

        keys = wide(level_near) * col_count + (wide(column_near) - col_start)
        local_row = wide(row_near) - row_start
        amount = wide(value_near)
        width = keys.shape[1]
        high = amount.astype(bf16).astype(f32)
        low = amount - high
        row_hot = lax.broadcasted_iota(jnp.int32, (row_count, width), 0) == local_row
        right = jnp.concatenate(
            [jnp.where(row_hot, high, 0.0).astype(bf16), jnp.where(row_hot, low, 0.0).astype(bf16)], axis=0
        )
        cells = lax.broadcasted_iota(jnp.int32, (col_count, width), 0)
        for idx in range(half):
            left = jnp.where(cells == keys - owned(idx, mem) * col_count, 1.0, 0.0).astype(bf16)
            hits[idx] += lax.dot_general(
                left, right, (((1,), (1,)), ((), ())), preferred_element_type=f32
            )

    def innov_copy(idx):
        lev = owned(idx, mem)
        return remote(
            innov_own.at[idx], innov_all.at[0, lon], innov_ss.at[idx], innov_rs.at[lon], device(lat, lev, mem)
        )

    for idx in range(half):
        block = (hits[idx, :, :row_count] + hits[idx, :, row_count:]).astype(bf16)
        innov_own[idx] = block
        lev = owned(idx, mem)
        pl.when(lev != lon)(lambda idx=idx: innov_copy(idx).start())

        @pl.when(lev == lon)
        def _(block=block):
            innov_all[0, lon] = block

    for slot in range(lead, lat_size):
        send_fields(0, slot)
    near_copies[4].wait()
    share, share_pad = taper_near.shape[0] // 4, taper_all.shape[2]
    modes_half = taper_near.shape[1] // 2
    spread = (4 * share_pad, 4 * share)
    out_row = lax.broadcasted_iota(jnp.int32, spread, 0)
    in_row = lax.broadcasted_iota(jnp.int32, spread, 1)
    chosen = jnp.zeros(spread, jnp.bool_)
    for idx, kind in enumerate(CLASSES):
        local_row = out_row - idx * share_pad
        chosen |= (local_row >= 0) & (local_row < share) & (in_row == 4 * local_row + kind)
    by_class = jnp.dot(
        jnp.where(chosen, 1.0, 0.0).astype(bf16), taper_near[...].astype(bf16), preferred_element_type=f32
    ).astype(bf16)
    for idx in range(4):
        taper_all[idx, lat] = by_class[idx * share_pad:(idx + 1) * share_pad]
    lanes = pl.ds(pl.multiple_of(mem * modes_half, modes_half), modes_half)

    def taper_copy(step):
        part = taper_all.at[:, lat, :, lanes]
        return remote(
            part, part, taper_ss.at[step], taper_rs.at[step], device(lax.rem(lat + step, lat_size), lon, mem)
        )

    def trade_copy(step):
        part = taper_all.at[:, lax.rem(lat + lat_size - step, lat_size), :, lanes]
        return remote(part, part, trade_ss.at[step], trade_rs.at[step], partner)

    for step in range(1, lat_size):
        taper_copy(step).start()
    for copy in near_copies[5:]:
        copy.wait()

    outer, inner = high_near.shape[2], low_near.shape[1]
    points, kind_size = even_inv.shape[1:]
    span = outer * inner
    low_cos, low_sin = low_near[0], low_near[1]
    fine[span:, :] = jnp.zeros((points - span, 4 * kind_size), f32)
    for block in range(2):
        first = 2 * block * kind_size
        for idx in range(outer):
            fine[idx * inner:(idx + 1) * inner, first:] = (
                high_near[0, block, idx:idx + 1, first:] * low_cos[:, first:]
                + high_near[1, block, idx:idx + 1, first:] * low_sin[:, first:]
            )
        for kind in range(2 * block, 4):
            tile = fine[:, kind * kind_size:(kind + 1) * kind_size]
            if kind < 2:
                even_inv[kind] = tile.astype(bf16)
                even_fwd[kind] = tile.T.astype(bf16)
            else:
                rows = slice(block * points, (block + 1) * points)
                cols = slice((kind - 2) * kind_size, (kind - 1) * kind_size)
                odd_inv[rows, cols] = tile.astype(bf16)
                odd_fwd[cols, rows] = tile.T.astype(bf16)
    folded[...] = jnp.zeros_like(folded)

    lat_inner = lat_low_near.shape[1]
    per_band = row_count // lat_inner
    lat_cos, lat_sin = lat_low_near[0], lat_low_near[1]
    for slot in range(lat_size):
        band = lax.rem(lat + lat_size - slot, lat_size)
        for idx in range(per_band):
            spot = pl.ds(band * per_band + idx, 1)
            rows = slice(slot * row_count + idx * lat_inner, slot * row_count + (idx + 1) * lat_inner)
            modes[rows, :] = (
                lat_high_near[0, spot, :] * lat_cos - lat_high_near[1, spot, :] * lat_sin
            ).astype(bf16)

    def gather_copy(slot):
        return remote(
            innov_all.at[0], innov_all.at[slot], gather_ss.at[slot], gather_rs.at[slot],
            device(lax.rem(lat + slot, lat_size), lon, mem),
        )

    def share_copy(slot):
        return remote(innov_all.at[slot], innov_all.at[slot], share_ss.at[slot], share_rs.at[slot], partner)

    send_fields(1, 0)

    @pl.when(receives)
    def _():
        for step in range(1, lon_size):
            sender = lax.rem(lon + step, lon_size)
            remote(
                innov_own.at[0], innov_all.at[0, sender], innov_ss.at[0], innov_rs.at[sender],
                device(lat, sender, mem),
            ).wait_recv()
        for slot in range(1, lat_size):
            gather_copy(slot).start()
        share_copy(0).start()

    for turn in range(1, own):
        for slot in range(1 if turn == 1 else 0, lat_size):
            send_fields(turn, slot)

    @pl.when(receives)
    def _():
        for slot in range(1, lat_size):
            gather_copy(slot).wait_recv()
            share_copy(slot).start()

    @pl.when(jnp.logical_not(receives))
    def _():
        for slot in range(lat_size):
            share_copy(slot).wait_recv()

    total[...] = jnp.zeros_like(total)
    for step in range(1, lat_size):
        taper_copy(step).wait_recv()
        trade_copy(step).start()
    for step in range(1, lat_size):
        trade_copy(step).wait_recv()

    stages = lat_size // 2
    pair = 2 * row_count
    fourth = lon_size // 4
    kinds = 4 * kind_size

    def fold(turn, slot, lanes):
        def quarter_of(which):
            parts = []
            for idx in range(fourth):
                block = which * fourth + idx
                parts.append(fields[turn, slot, block].astype(f32) * innov_all[slot, block].astype(f32))
            return parts[0] if fourth == 1 else jnp.concatenate(parts, axis=0)

        first, second, third, last = [quarter_of(which) for which in range(4)]
        even, odd = first + third, second + last
        for idx, value in enumerate([even + odd, even - odd, first - third, second - last]):
            folded[pl.ds(idx * points, span), lanes] = value.astype(bf16)

    def zonal_of(turn, stage):
        for which in range(2):
            slot = 2 * stage + which

            @pl.loop(0, lon_size)
            def _(step, slot=slot):
                pl.when(slot + step == 0)(lambda: own_copy(turn).wait())
                pl.when(slot + step > 0)(lambda: field_copy(turn, slot, step).wait_recv())

            fold(turn, slot, slice(which * row_count, (which + 1) * row_count))
        for kind in range(2):
            zonal[kind * kind_size:(kind + 1) * kind_size, :] = jnp.dot(
                even_fwd[kind], folded[kind * points:(kind + 1) * points, :], preferred_element_type=f32
            ).astype(bf16)
        zonal[2 * kind_size:, :] = jnp.dot(
            odd_fwd[...], folded[2 * points:, :], preferred_element_type=f32
        ).astype(bf16)
        return jnp.dot(zonal[...], modes[stage * pair:(stage + 1) * pair, :], preferred_element_type=f32)

    def transform(turn):
        for stage in range(stages - 1):
            terms = zonal_of(turn, stage)
            spectrum[...] = terms if stage == 0 else spectrum[...] + terms
        terms = zonal_of(turn, stages - 1) + spectrum[...]
        tapered[...] = (terms * taper_all[...].reshape(kinds, lat_size * row_count).astype(f32)).astype(bf16)

    def localize(turn, stage):
        inverse[...] = lax.dot_general(
            tapered[...], modes[pl.ds(pl.multiple_of(stage * pair, pair), pair), :],
            (((1,), (1,)), ((), ())), preferred_element_type=f32,
        ).astype(bf16)

        def back(table, rows):
            return jnp.dot(table, inverse[rows, :], preferred_element_type=f32)

        even = back(even_inv[0, :span], slice(0, kind_size))
        swing = back(even_inv[1, :span], slice(kind_size, 2 * kind_size))
        odd = [back(odd_inv[idx * points:idx * points + span, :], slice(2 * kind_size, kinds)) for idx in range(2)]
        for which in range(4):
            base = even + swing if which % 2 == 0 else even - swing
            values = base + odd[which % 2] if which < 2 else base - odd[which % 2]
            for idx in range(fourth):
                block = which * fourth + idx
                for part in range(2):
                    slot = 2 * stage + part
                    total[block, slot] += (
                        fields[turn, slot, block].astype(f32)
                        * values[idx * col_count:(idx + 1) * col_count, part * row_count:(part + 1) * row_count]
                    )

    @pl.loop(0, own - 1)
    def _(turn):
        transform(turn)
        pl.loop(0, stages)(lambda stage: localize(turn, stage))

    transform(own - 1)

    def mem_copy(idx, stage):
        slots = pl.ds(2 * stage, 2)
        return remote(
            total.at[owned(idx, 1 - mem), slots], partner_part.at[idx, slots],
            mem_ss.at[idx, stage], mem_rs.at[idx, stage], partner,
        )

    @pl.loop(0, stages)
    def _(step):
        stage = stages - 1 - step
        localize(own - 1, stage)
        for idx in range(half):
            mem_copy(idx, stage).start()

    cutoff = col_count // 2 // 16 * 16
    bands = [slice(0, cutoff), slice(cutoff, col_count)]

    def lat_copy(idx, slot, band):
        rows = bands[band]
        return remote(
            lat_send.at[idx, slot, rows], lat_recv.at[idx, slot, rows],
            lat_ss.at[idx, slot, band], lat_rs.at[idx, slot, band],
            device(lax.rem(lat + lat_size - slot, lat_size), lon, mem),
        )

    def near_copy(idx, slot):
        return remote(
            near_send.at[idx, slot], near_recv.at[lax.rem(lon, half), slot],
            near_ss.at[idx, slot], near_rs.at[lax.rem(lon, half), slot],
            device(lax.rem(lat + lat_size - slot, lat_size), owned(quarter + idx, mem), mem),
        )

    slots = range(lat_size - 1, -1, -1)
    for idx in range(quarter):
        block = owned(idx, mem)
        for band in range(2):
            for slot in slots:
                if band == 0 and slot % 2 == 1:
                    mem_copy(idx, slot // 2).wait_recv()
                rows = bands[band]
                lat_send[idx, slot, rows] = (total[block, slot, rows] + partner_part[idx, slot, rows]).astype(bf16)
                if slot > 0:
                    lat_copy(idx, slot, band).start()
    for idx in range(quarter):
        block = owned(quarter + idx, mem)
        for slot in slots:
            if slot % 2 == 1:
                mem_copy(quarter + idx, slot // 2).wait_recv()
            value = (total[block, slot] + partner_part[quarter + idx, slot]).astype(bf16)
            if slot > 0:
                near_send[idx, slot] = value
                near_copy(idx, slot).start()
            else:
                @pl.when(block != lon)
                def _(idx=idx, value=value):
                    near_send[idx, 0] = value
                    near_copy(idx, 0).start()

                @pl.when(block == lon)
                def _(value=value):
                    near_recv[lax.rem(lon, half), 0] = value

    def lon_copy(idx, band):
        rows = bands[band]
        return remote(
            lon_send.at[idx, rows], lon_recv.at[lon, rows], lon_ss.at[idx, band], lon_rs.at[lon, band],
            device(lat, owned(idx, mem), mem),
        )

    for band in range(2):
        rows = bands[band]
        for idx in range(quarter):
            summed = lat_send[idx, 0, rows].astype(f32)
            for slot in range(1, lat_size):
                lat_copy(idx, slot, band).wait_recv()
                summed += lat_recv[idx, slot, rows].astype(f32)
            lon_send[idx, rows] = summed.astype(bf16)
            lon_copy(idx, band).start()

    def pair_copy(sender):
        return remote(lon_recv.at[sender], out.at[sender], pair_ss.at[sender], pair_rs.at[sender], partner)

    def out_copy(sender):
        return pltpu.make_async_copy(lon_recv.at[sender], out.at[sender], out_sem.at[sender])

    far = [(1 - side) * half + idx for idx in range(half)]
    close = [side * half + lax.rem(lon + idx, half) for idx in range(half)]

    @pl.when(receives)
    def _():
        for idx, sender in enumerate(close):
            local_level = lax.rem(lon + idx, half)
            summed = None
            for slot in range(lat_size):
                if idx + slot > 0:
                    remote(
                        near_send.at[0, slot], near_recv.at[local_level, slot], near_ss.at[0, slot],
                        near_rs.at[local_level, slot], device(lax.rem(lat + slot, lat_size), sender, mem),
                    ).wait_recv()
                term = near_recv[local_level, slot].astype(f32)
                summed = term if slot == 0 else summed + term
            lon_recv[sender] = summed.astype(bf16)
            pair_copy(sender).start()
            out_copy(sender).start()
        for sender in far:
            for band in range(2):
                rows = bands[band]
                remote(
                    lon_send.at[0, rows], lon_recv.at[sender, rows], lon_ss.at[0, band], lon_rs.at[sender, band],
                    device(lat, sender, mem),
                ).wait_recv()
            pair_copy(sender).start()
            out_copy(sender).start()

    @pl.when(jnp.logical_not(receives))
    def _():
        for sender in close + far:
            pair_copy(sender).wait_recv()

    @pl.when(receives)
    def _():
        for sender in close + far:
            pair_copy(sender).wait_send()
            out_copy(sender).wait()
        for slot in range(1, lat_size):
            gather_copy(slot).wait_send()
        for slot in range(lat_size):
            share_copy(slot).wait_send()

    for idx in range(half):
        pl.when(owned(idx, mem) != lon)(lambda idx=idx: innov_copy(idx).wait_send())
        for stage in range(stages):
            mem_copy(idx, stage).wait_send()
    for idx in range(quarter):
        for band in range(2):
            lon_copy(idx, band).wait_send()
            for slot in range(1, lat_size):
                lat_copy(idx, slot, band).wait_send()
        for slot in range(1, lat_size):
            near_copy(idx, slot).wait_send()
        pl.when(owned(quarter + idx, mem) != lon)(lambda idx=idx: near_copy(idx, 0).wait_send())
    for step in range(1, lat_size):
        taper_copy(step).wait_send()
        trade_copy(step).wait_send()

    @pl.loop(0, own)
    def _(turn):
        for slot in range(lat_size):
            @pl.loop(1 if slot == 0 else 0, lon_size)
            def _(step, slot=slot):
                field_copy(turn, slot, step).wait_send()


def local(anomalies, taper, obs_row, obs_col, obs_level, obs_value):
    member_count, level_count, col_count, row_count = anomalies.shape
    lon_size, lat_size = lax.axis_size("lon"), lax.axis_size("lat")
    lat_total = row_count * lat_size
    ensemble = member_count * lax.axis_size("mem")
    own = member_count // lat_size
    half = lon_size // 2
    part_count = taper.shape[1]
    lon_total = col_count * lon_size
    seeds = lon_seeds(lon_total, lat_size) + lat_seeds(lat_total)
    share_pad = round_up(part_count // 4, 16)
    kind_size, points = lat_size * share_pad, round_up(lon_total // 4, 128)
    f32, bf16 = jnp.float32, jnp.bfloat16
    slab = (col_count, row_count)
    whole = pl.BlockSpec(memory_space=pl.ANY)
    dma = pltpu.SemaphoreType.DMA
    obs = [(table.shape, table.dtype) for table in (obs_level, obs_col, obs_row, obs_value)]
    near = obs + [(seed.shape, f32) for seed in seeds]
    result = pl.pallas_call(
        functools.partial(fused_kernel, lat_size, lon_size, own, obs_row.shape[0]),
        out_shape=jax.ShapeDtypeStruct((level_count,) + slab, bf16),
        in_specs=[whole] * 10,
        out_specs=whole,
        scratch_shapes=[
            pltpu.VMEM((own, lat_size, lon_size) + slab, bf16),
            pltpu.VMEM((2, kind_size, points), bf16),
            pltpu.VMEM((2 * kind_size, 2 * points), bf16),
            pltpu.VMEM((2, points, kind_size), bf16),
            pltpu.VMEM((2 * points, 2 * kind_size), bf16),
            pltpu.VMEM((points, 4 * kind_size), f32),
            pltpu.VMEM((lat_total, lat_total), bf16),
            pltpu.VMEM((part_count, lat_total), f32),
            pltpu.VMEM((4, lat_size, share_pad, lat_total), bf16),
            pltpu.VMEM((half, col_count, 2 * row_count), f32),
            pltpu.VMEM((half,) + slab, bf16),
            pltpu.VMEM((lat_size, lon_size) + slab, bf16),
            pltpu.VMEM((4 * points, 2 * row_count), bf16),
            pltpu.VMEM((4 * kind_size, 2 * row_count), bf16),
            pltpu.VMEM((4 * kind_size, lat_total), f32),
            pltpu.VMEM((4 * kind_size, lat_total), bf16),
            pltpu.VMEM((4 * kind_size, 2 * row_count), bf16),
            pltpu.VMEM((lon_size, lat_size) + slab, f32),
            pltpu.VMEM((half, lat_size) + slab, f32),
            pltpu.VMEM((half // 2, lat_size) + slab, bf16),
            pltpu.VMEM((half // 2, lat_size) + slab, bf16),
            pltpu.VMEM((half // 2, lat_size) + slab, bf16),
            pltpu.VMEM((half, lat_size) + slab, bf16),
            pltpu.VMEM((half // 2,) + slab, bf16),
            pltpu.VMEM((level_count,) + slab, bf16),
            *[pltpu.VMEM(shape, dtype) for shape, dtype in near],
            dma((own, lat_size, lon_size)), dma((own, lat_size, lon_size)), dma((own,)), dma((9,)),
            dma((lat_size,)), dma((lat_size,)), dma((lat_size,)), dma((lat_size,)), dma((half,)), dma((lon_size,)),
            dma((lat_size,)), dma((lat_size,)), dma((lat_size,)), dma((lat_size,)),
            dma((half, lat_size // 2)), dma((half, lat_size // 2)), dma((half // 2, lat_size, 2)),
            dma((half // 2, lat_size, 2)), dma((half // 2, lat_size)), dma((half, lat_size)),
            dma((half // 2, 2)), dma((lon_size, 2)), dma((lon_size,)), dma((lon_size,)), dma((lon_size,)),
        ],
        compiler_params=pltpu.CompilerParams(
            collective_id=0, has_side_effects=True, vmem_limit_bytes=60 * 1024 * 1024
        ),
    )(
        anomalies, taper, obs_level, obs_col, obs_row, obs_value, *seeds,
    )
    return result.astype(f32) / (ensemble - 1)


def solution(mesh):
    in_specs = (
        P("mem", None, "lon", "lat"),
        P("lon", "lat", None),
        P("lat", "lon"),
        P("lat", "lon"),
        P("lat", "lon"),
        P("lat", "lon"),
    )
    out_specs = P(None, "lon", "lat")
    return jax.shard_map(local, mesh=mesh, in_specs=in_specs, out_specs=out_specs, check_vma=False)
```

```python
import functools
import math

import jax
import jax.numpy as jnp
import numpy as np
from jax import lax
from jax.experimental import pallas as pl
from jax.experimental.pallas import tpu as pltpu
from jax.sharding import PartitionSpec as P


CLASSES = (0, 2, 1, 3)


def round_up(size, unit):
    return -(-size // unit) * unit


def lon_seeds(length, part_count):
    nyquist = length // 2
    quarter = length // 4
    inner = next(n for n in range(24, 0, -8) if quarter % n == 0)
    outer = quarter // inner
    share = quarter // part_count
    padded = round_up(share, 16)
    offsets = np.arange(padded)
    coef_idx = np.stack([
        np.stack([part * (length // part_count) + 4 * offsets + kind for part in range(part_count)])
        for kind in CLASSES
    ])
    real = np.broadcast_to(offsets < share, coef_idx.shape).reshape(-1)
    coef_idx = np.where(real, coef_idx.reshape(-1), 0)
    wavenum = np.where(coef_idx <= nyquist, coef_idx, coef_idx - nyquist)

    def waves(points):
        angles = (points[:, None] * wavenum[None, :] % length) * (2.0 * math.pi / length)
        return np.cos(angles), np.sin(angles)

    scales = np.where((coef_idx == 0) | (coef_idx == nyquist), 1.0 / math.sqrt(length), math.sqrt(2.0 / length))
    scales = np.where(real, scales, 0.0)
    is_cos = coef_idx <= nyquist
    starts = np.arange(2)[:, None] * quarter + np.arange(outer)[None, :] * inner
    high_cos, high_sin = waves(starts.reshape(-1))
    first = np.where(is_cos, high_cos, high_sin) * scales
    second = np.where(is_cos, -high_sin, high_cos) * scales
    high = np.stack([first, second]).reshape(2, 2, outer, -1)
    low = np.stack(waves(np.arange(inner)))
    return [jnp.asarray(part, jnp.float32) for part in (high, low)]


def lat_seeds(length):
    inner = next(size for size in range(32, 0, -1) if length % size == 0)
    outer = length // inner
    mode_idx = np.arange(length)[None, :]

    def waves(points):
        angles = (mode_idx * points[:, None] % (4 * length)) * (math.pi / (2.0 * length))
        return np.cos(angles), np.sin(angles)

    scales = np.where(mode_idx == 0, 1.0 / math.sqrt(length), math.sqrt(2.0 / length))
    high = np.stack(waves(np.arange(outer) * (2 * inner))) * scales
    low = np.stack(waves(np.arange(inner) * 2 + 1))
    return [jnp.asarray(part, jnp.float32) for part in (high, low)]


def fused_kernel(
    lat_size, lon_size, own, obs_rows,
    anom, taper, level, column, row, value, lon_high, lon_low, lat_high, lat_low, out,
    fields, even_fwd, odd_fwd, even_inv, odd_inv, fine, modes, taper_near, taper_all, far_send, far_recv, far_near, far_hits, hits, innov_own, innov_all,
    folded, zonal, spectrum, tapered, inverse, total, partner_part, lat_send, lat_recv, near_send, near_recv, lon_send, lon_recv,
    level_near, column_near, row_near, value_near, high_near, low_near, lat_high_near, lat_low_near,
    field_ss, field_rs, local_sem, table_sem, taper_ss, taper_rs, trade_ss, trade_rs, far_ss, far_rs, innov_ss, innov_rs,
    gather_ss, gather_rs, share_ss, share_rs, mem_ss, mem_rs, lat_ss, lat_rs, near_ss, near_rs, lon_ss, lon_rs, pair_ss, pair_rs, out_sem,
):
    lat, lon, mem = lax.axis_index("lat"), lax.axis_index("lon"), lax.axis_index("mem")
    place_count = lat_size * lon_size
    half = lon_size // 2
    quarter = half // 2
    me = lat * lon_size + lon
    side = lax.div(lon, half)
    receives = lax.div(lax.rem(lon, half), quarter) == mem
    col_count, row_count = fields.shape[3:]
    f32, bf16 = jnp.float32, jnp.bfloat16

    def device(lat_idx, lon_idx, mem_idx):
        return {"lat": lat_idx, "lon": lon_idx, "mem": mem_idx}

    partner = device(lat, lon, 1 - mem)

    def remote(src, dst, send, recv, target):
        return pltpu.make_async_remote_copy(
            src_ref=src, dst_ref=dst, send_sem=send, recv_sem=recv,
            device_id=target, device_id_type=pl.DeviceIdType.MESH,
        )

    def owned(idx, core):
        near = lax.div(idx, quarter)
        return (1 - side + near * (2 * side - 1)) * half + core * quarter + lax.rem(idx, quarter)

    near_copies = [
        pltpu.make_async_copy(src, dst, table_sem.at[idx])
        for idx, (src, dst) in enumerate([
            (level, level_near), (column, column_near), (row, row_near), (value, value_near),
            (taper.at[0], taper_near), (lon_high, high_near), (lon_low, low_near),
            (lat_high, lat_high_near), (lat_low, lat_low_near),
        ])
    ]
    for copy in near_copies:
        copy.start()
    col_start, row_start = lon * col_count, lat * row_count
    for copy in near_copies[:4]:
        copy.wait()

    local_col = column_near[...] - col_start
    pairs = lax.shift_right_logical(local_col, 1).astype(f32).astype(bf16)
    parities = (2 * (row_near[...] - row_start) + lax.bitwise_and(local_col, 1)).astype(f32).astype(bf16)
    for idx in range(quarter):
        far_send[idx, 0] = jnp.where(level_near[...] == owned(idx, mem), value_near[...], 0.0).astype(bf16)
        far_send[idx, 1] = pairs
        far_send[idx, 2] = parities

    barrier = pltpu.get_barrier_semaphore()

    @pl.loop(1, place_count)
    def _(offset):
        spot = lax.rem(me + offset, place_count)
        pl.semaphore_signal(
            barrier, inc=1, device_id=device(lax.div(spot, lon_size), lax.rem(spot, lon_size), mem),
            device_id_type=pl.DeviceIdType.MESH,
        )

    pl.semaphore_signal(barrier, inc=1, device_id=partner, device_id_type=pl.DeviceIdType.MESH)
    pl.semaphore_wait(barrier, place_count)

    def far_copy(idx):
        return remote(
            far_send.at[idx], far_recv.at[lax.rem(lon, half)], far_ss.at[idx], far_rs.at[lax.rem(lon, half)],
            device(lat, owned(idx, mem), mem),
        )

    for idx in range(quarter):
        far_copy(idx).start()

    def field_copy(turn, slot, step):
        lat_idx, lon_idx = lax.rem(lat + slot, lat_size), lax.rem(lon + step, lon_size)
        return remote(
            anom.at[lat_idx * own + turn, lon_idx], fields.at[turn, slot, lon],
            field_ss.at[turn, slot, step], field_rs.at[turn, slot, step], device(lat_idx, lon_idx, mem),
        )

    def send_fields(turn, slot):
        @pl.loop(0, lon_size - 1 if slot == 0 else lon_size)
        def _(idx):
            step = half + lax.div(idx + 1, 2) * (1 - 2 * lax.rem(idx, 2))
            field_copy(turn, slot, step).start()

    def own_copy(turn):
        return pltpu.make_async_copy(
            anom.at[lat * own + turn, lon], fields.at[turn, 0, lon], local_sem.at[turn]
        )

    lead = lat_size // 2
    for slot in range(lead):
        send_fields(0, slot)
    for turn in range(own):
        own_copy(turn).start()

    hits[...] = jnp.zeros_like(hits)
    group = 4

    @pl.loop(0, obs_rows // group)
    def _(step):
        def wide(ref):
            return jnp.concatenate([ref[pl.ds(step * group + part, 1), :] for part in range(group)], axis=1)

        keys = wide(level_near) * col_count + (wide(column_near) - col_start)
        local_row = wide(row_near) - row_start
        amount = wide(value_near)
        width = keys.shape[1]
        high = amount.astype(bf16).astype(f32)
        low = amount - high
        row_hot = lax.broadcasted_iota(jnp.int32, (row_count, width), 0) == local_row
        right = jnp.concatenate(
            [jnp.where(row_hot, high, 0.0).astype(bf16), jnp.where(row_hot, low, 0.0).astype(bf16)], axis=0
        )
        cells = lax.broadcasted_iota(jnp.int32, (col_count, width), 0)
        for idx in range(quarter):
            left = jnp.where(cells == keys - owned(quarter + idx, mem) * col_count, 1.0, 0.0).astype(bf16)
            hits[idx] += lax.dot_general(
                left, right, (((1,), (1,)), ((), ())), preferred_element_type=f32
            )

    def innov_copy(idx):
        lev = owned(quarter + idx, mem)
        return remote(
            innov_own.at[idx], innov_all.at[0, lon], innov_ss.at[idx], innov_rs.at[lon], device(lat, lev, mem)
        )

    for idx in range(quarter):
        block = (hits[idx, :, :row_count] + hits[idx, :, row_count:]).astype(bf16)
        innov_own[idx] = block
        lev = owned(quarter + idx, mem)
        pl.when(lev != lon)(lambda idx=idx: innov_copy(idx).start())

        @pl.when(lev == lon)
        def _(block=block):
            innov_all[0, lon] = block

    for slot in range(lead, lat_size):
        send_fields(0, slot)
    def gather_copy(slot):
        return remote(
            innov_all.at[0], innov_all.at[slot], gather_ss.at[slot], gather_rs.at[slot],
            device(lax.rem(lat + slot, lat_size), lon, mem),
        )

    def share_copy(slot):
        return remote(innov_all.at[slot], innov_all.at[slot], share_ss.at[slot], share_rs.at[slot], partner)

    @pl.when(receives)
    def _():
        @pl.loop(0, half)
        def _(source):
            remote(
                far_send.at[0], far_recv.at[source], far_ss.at[0], far_rs.at[source],
                device(lat, (1 - side) * half + source, mem),
            ).wait_recv()
            far_near[...] = far_recv[source].astype(f32)
            far_hits[...] = jnp.zeros_like(far_hits)

            @pl.loop(0, obs_rows // group)
            def _(step):
                def wide(kind):
                    return jnp.concatenate(
                        [far_near[kind, pl.ds(step * group + part, 1), :] for part in range(group)], axis=1
                    )

                coded = wide(2).astype(jnp.int32)
                local_row = lax.shift_right_logical(coded, 1)
                local_col = 2 * wide(1).astype(jnp.int32) + lax.bitwise_and(coded, 1)
                width = coded.shape[1]
                row_hot = lax.broadcasted_iota(jnp.int32, (row_count, width), 0) == local_row
                right = jnp.where(row_hot, wide(0), 0.0).astype(bf16)
                cells = lax.broadcasted_iota(jnp.int32, (col_count, width), 0)
                left = jnp.where(cells == local_col, 1.0, 0.0).astype(bf16)
                far_hits[...] += lax.dot_general(
                    left, right, (((1,), (1,)), ((), ())), preferred_element_type=f32
                )

            innov_all[0, (1 - side) * half + source] = far_hits[...].astype(bf16)

        for idx in range(1, half):
            sender = side * half + lax.rem(lon + idx, half)
            remote(
                innov_own.at[0], innov_all.at[0, sender], innov_ss.at[0], innov_rs.at[sender],
                device(lat, sender, mem),
            ).wait_recv()
        for slot in range(1, lat_size):
            gather_copy(slot).start()
        share_copy(0).start()

    near_copies[4].wait()
    share, share_pad = taper_near.shape[0] // 4, taper_all.shape[2]
    modes_half = taper_near.shape[1] // 2
    spread = (4 * share_pad, 4 * share)
    out_row = lax.broadcasted_iota(jnp.int32, spread, 0)
    in_row = lax.broadcasted_iota(jnp.int32, spread, 1)
    chosen = jnp.zeros(spread, jnp.bool_)
    for idx, kind in enumerate(CLASSES):
        local_row = out_row - idx * share_pad
        chosen |= (local_row >= 0) & (local_row < share) & (in_row == 4 * local_row + kind)
    by_class = jnp.dot(
        jnp.where(chosen, 1.0, 0.0).astype(bf16), taper_near[...].astype(bf16), preferred_element_type=f32
    ).astype(bf16)
    for idx in range(4):
        taper_all[idx, lat] = by_class[idx * share_pad:(idx + 1) * share_pad]
    lanes = pl.ds(pl.multiple_of(mem * modes_half, modes_half), modes_half)

    def taper_copy(step):
        part = taper_all.at[:, lat, :, lanes]
        return remote(
            part, part, taper_ss.at[step], taper_rs.at[step], device(lax.rem(lat + step, lat_size), lon, mem)
        )

    def trade_copy(step):
        part = taper_all.at[:, lax.rem(lat + lat_size - step, lat_size), :, lanes]
        return remote(part, part, trade_ss.at[step], trade_rs.at[step], partner)

    for step in range(1, lat_size):
        taper_copy(step).start()

    for turn in range(1, own):
        for slot in range(lat_size):
            send_fields(turn, slot)

    for copy in near_copies[5:]:
        copy.wait()

    outer, inner = high_near.shape[2], low_near.shape[1]
    points, kind_size = even_inv.shape[1:]
    span = outer * inner
    low_cos, low_sin = low_near[0], low_near[1]
    fine[span:, :] = jnp.zeros((points - span, 4 * kind_size), f32)
    for block in range(2):
        first = 2 * block * kind_size
        for idx in range(outer):
            fine[idx * inner:(idx + 1) * inner, first:] = (
                high_near[0, block, idx:idx + 1, first:] * low_cos[:, first:]
                + high_near[1, block, idx:idx + 1, first:] * low_sin[:, first:]
            )
        for kind in range(2 * block, 4):
            tile = fine[:, kind * kind_size:(kind + 1) * kind_size]
            if kind < 2:
                even_inv[kind] = tile.astype(bf16)
                even_fwd[kind] = tile.T.astype(bf16)
            else:
                rows = slice(block * points, (block + 1) * points)
                cols = slice((kind - 2) * kind_size, (kind - 1) * kind_size)
                odd_inv[rows, cols] = tile.astype(bf16)
                odd_fwd[cols, rows] = tile.T.astype(bf16)
    folded[...] = jnp.zeros_like(folded)

    lat_inner = lat_low_near.shape[1]
    per_band = row_count // lat_inner
    lat_cos, lat_sin = lat_low_near[0], lat_low_near[1]
    for slot in range(lat_size):
        band = lax.rem(lat + lat_size - slot, lat_size)
        for idx in range(per_band):
            spot = pl.ds(band * per_band + idx, 1)
            rows = slice(slot * row_count + idx * lat_inner, slot * row_count + (idx + 1) * lat_inner)
            modes[rows, :] = (
                lat_high_near[0, spot, :] * lat_cos - lat_high_near[1, spot, :] * lat_sin
            ).astype(bf16)

    @pl.when(receives)
    def _():
        for slot in range(1, lat_size):
            gather_copy(slot).wait_recv()
            share_copy(slot).start()

    @pl.when(jnp.logical_not(receives))
    def _():
        for slot in range(lat_size):
            share_copy(slot).wait_recv()

    total[...] = jnp.zeros_like(total)
    for step in range(1, lat_size):
        taper_copy(step).wait_recv()
        trade_copy(step).start()
    for step in range(1, lat_size):
        trade_copy(step).wait_recv()

    stages = lat_size // 2
    pair = 2 * row_count
    fourth = lon_size // 4
    kinds = 4 * kind_size

    def fold(turn, slot, lanes):
        def quarter_of(which):
            parts = []
            for idx in range(fourth):
                block = which * fourth + idx
                parts.append(fields[turn, slot, block].astype(f32) * innov_all[slot, block].astype(f32))
            return parts[0] if fourth == 1 else jnp.concatenate(parts, axis=0)

        first, second, third, last = [quarter_of(which) for which in range(4)]
        even, odd = first + third, second + last
        for idx, value in enumerate([even + odd, even - odd, first - third, second - last]):
            folded[pl.ds(idx * points, span), lanes] = value.astype(bf16)

    def zonal_of(turn, stage):
        for which in range(2):
            slot = 2 * stage + which

            @pl.loop(0, lon_size)
            def _(step, slot=slot):
                pl.when(slot + step == 0)(lambda: own_copy(turn).wait())
                pl.when(slot + step > 0)(lambda: field_copy(turn, slot, step).wait_recv())

            fold(turn, slot, slice(which * row_count, (which + 1) * row_count))
        for kind in range(2):
            zonal[kind * kind_size:(kind + 1) * kind_size, :] = jnp.dot(
                even_fwd[kind], folded[kind * points:(kind + 1) * points, :], preferred_element_type=f32
            ).astype(bf16)
        zonal[2 * kind_size:, :] = jnp.dot(
            odd_fwd[...], folded[2 * points:, :], preferred_element_type=f32
        ).astype(bf16)
        return jnp.dot(zonal[...], modes[stage * pair:(stage + 1) * pair, :], preferred_element_type=f32)

    def transform(turn):
        for stage in range(stages - 1):
            terms = zonal_of(turn, stage)
            spectrum[...] = terms if stage == 0 else spectrum[...] + terms
        terms = zonal_of(turn, stages - 1) + spectrum[...]
        tapered[...] = (terms * taper_all[...].reshape(kinds, lat_size * row_count).astype(f32)).astype(bf16)

    def localize(turn, stage):
        inverse[...] = lax.dot_general(
            tapered[...], modes[pl.ds(pl.multiple_of(stage * pair, pair), pair), :],
            (((1,), (1,)), ((), ())), preferred_element_type=f32,
        ).astype(bf16)

        def back(table, rows):
            return jnp.dot(table, inverse[rows, :], preferred_element_type=f32)

        even = back(even_inv[0, :span], slice(0, kind_size))
        swing = back(even_inv[1, :span], slice(kind_size, 2 * kind_size))
        odd = [back(odd_inv[idx * points:idx * points + span, :], slice(2 * kind_size, kinds)) for idx in range(2)]
        for which in range(4):
            base = even + swing if which % 2 == 0 else even - swing
            values = base + odd[which % 2] if which < 2 else base - odd[which % 2]
            for idx in range(fourth):
                block = which * fourth + idx
                for part in range(2):
                    slot = 2 * stage + part
                    total[block, slot] += (
                        fields[turn, slot, block].astype(f32)
                        * values[idx * col_count:(idx + 1) * col_count, part * row_count:(part + 1) * row_count]
                    )

    @pl.loop(0, own - 1)
    def _(turn):
        transform(turn)
        pl.loop(0, stages)(lambda stage: localize(turn, stage))

    transform(own - 1)

    def mem_copy(idx, stage):
        slots = pl.ds(2 * stage, 2)
        return remote(
            total.at[owned(idx, 1 - mem), slots], partner_part.at[idx, slots],
            mem_ss.at[idx, stage], mem_rs.at[idx, stage], partner,
        )

    @pl.loop(0, stages)
    def _(step):
        stage = stages - 1 - step
        localize(own - 1, stage)
        for idx in range(half):
            mem_copy(idx, stage).start()

    cutoff = col_count // 2 // 16 * 16
    bands = [slice(0, cutoff), slice(cutoff, col_count)]

    def lat_copy(idx, slot, band):
        rows = bands[band]
        return remote(
            lat_send.at[idx, slot, rows], lat_recv.at[idx, slot, rows],
            lat_ss.at[idx, slot, band], lat_rs.at[idx, slot, band],
            device(lax.rem(lat + lat_size - slot, lat_size), lon, mem),
        )

    def near_copy(idx, slot):
        return remote(
            near_send.at[idx, slot], near_recv.at[lax.rem(lon, half), slot],
            near_ss.at[idx, slot], near_rs.at[lax.rem(lon, half), slot],
            device(lax.rem(lat + lat_size - slot, lat_size), owned(quarter + idx, mem), mem),
        )

    slots = range(lat_size - 1, -1, -1)
    for idx in range(quarter):
        block = owned(idx, mem)
        for band in range(2):
            for slot in slots:
                if band == 0 and slot % 2 == 1:
                    mem_copy(idx, slot // 2).wait_recv()
                rows = bands[band]
                lat_send[idx, slot, rows] = (total[block, slot, rows] + partner_part[idx, slot, rows]).astype(bf16)
                if slot > 0:
                    lat_copy(idx, slot, band).start()
    for idx in range(quarter):
        block = owned(quarter + idx, mem)
        for slot in slots:
            if slot % 2 == 1:
                mem_copy(quarter + idx, slot // 2).wait_recv()
            value = (total[block, slot] + partner_part[quarter + idx, slot]).astype(bf16)
            if slot > 0:
                near_send[idx, slot] = value
                near_copy(idx, slot).start()
            else:
                @pl.when(block != lon)
                def _(idx=idx, value=value):
                    near_send[idx, 0] = value
                    near_copy(idx, 0).start()

                @pl.when(block == lon)
                def _(value=value):
                    near_recv[lax.rem(lon, half), 0] = value

    def lon_copy(idx, band):
        rows = bands[band]
        return remote(
            lon_send.at[idx, rows], lon_recv.at[lon, rows], lon_ss.at[idx, band], lon_rs.at[lon, band],
            device(lat, owned(idx, mem), mem),
        )

    for band in range(2):
        rows = bands[band]
        for idx in range(quarter):
            summed = lat_send[idx, 0, rows].astype(f32)
            for slot in range(1, lat_size):
                lat_copy(idx, slot, band).wait_recv()
                summed += lat_recv[idx, slot, rows].astype(f32)
            lon_send[idx, rows] = summed.astype(bf16)
            lon_copy(idx, band).start()

    def pair_copy(sender):
        return remote(lon_recv.at[sender], out.at[sender], pair_ss.at[sender], pair_rs.at[sender], partner)

    def out_copy(sender):
        return pltpu.make_async_copy(lon_recv.at[sender], out.at[sender], out_sem.at[sender])

    far = [(1 - side) * half + idx for idx in range(half)]
    close = [side * half + lax.rem(lon + idx, half) for idx in range(half)]

    @pl.when(receives)
    def _():
        for idx, sender in enumerate(close):
            local_level = lax.rem(lon + idx, half)
            summed = None
            for slot in range(lat_size):
                if idx + slot > 0:
                    remote(
                        near_send.at[0, slot], near_recv.at[local_level, slot], near_ss.at[0, slot],
                        near_rs.at[local_level, slot], device(lax.rem(lat + slot, lat_size), sender, mem),
                    ).wait_recv()
                term = near_recv[local_level, slot].astype(f32)
                summed = term if slot == 0 else summed + term
            lon_recv[sender] = summed.astype(bf16)
            pair_copy(sender).start()
            out_copy(sender).start()
        for sender in far:
            for band in range(2):
                rows = bands[band]
                remote(
                    lon_send.at[0, rows], lon_recv.at[sender, rows], lon_ss.at[0, band], lon_rs.at[sender, band],
                    device(lat, sender, mem),
                ).wait_recv()
            pair_copy(sender).start()
            out_copy(sender).start()

    @pl.when(jnp.logical_not(receives))
    def _():
        for sender in close + far:
            pair_copy(sender).wait_recv()

    @pl.when(receives)
    def _():
        for sender in close + far:
            pair_copy(sender).wait_send()
            out_copy(sender).wait()
        for slot in range(1, lat_size):
            gather_copy(slot).wait_send()
        for slot in range(lat_size):
            share_copy(slot).wait_send()

    for idx in range(half):
        for stage in range(stages):
            mem_copy(idx, stage).wait_send()
    for idx in range(quarter):
        for band in range(2):
            lon_copy(idx, band).wait_send()
            for slot in range(1, lat_size):
                lat_copy(idx, slot, band).wait_send()
        for slot in range(1, lat_size):
            near_copy(idx, slot).wait_send()
        pl.when(owned(quarter + idx, mem) != lon)(lambda idx=idx: near_copy(idx, 0).wait_send())
        pl.when(owned(quarter + idx, mem) != lon)(lambda idx=idx: innov_copy(idx).wait_send())
        far_copy(idx).wait_send()
    for step in range(1, lat_size):
        taper_copy(step).wait_send()
        trade_copy(step).wait_send()

    @pl.loop(0, own)
    def _(turn):
        for slot in range(lat_size):
            @pl.loop(1 if slot == 0 else 0, lon_size)
            def _(step, slot=slot):
                field_copy(turn, slot, step).wait_send()


def local(anomalies, taper, obs_row, obs_col, obs_level, obs_value):
    member_count, level_count, col_count, row_count = anomalies.shape
    lon_size, lat_size = lax.axis_size("lon"), lax.axis_size("lat")
    lat_total = row_count * lat_size
    ensemble = member_count * lax.axis_size("mem")
    own = member_count // lat_size
    half = lon_size // 2
    part_count = taper.shape[1]
    lon_total = col_count * lon_size
    seeds = lon_seeds(lon_total, lat_size) + lat_seeds(lat_total)
    share_pad = round_up(part_count // 4, 16)
    kind_size, points = lat_size * share_pad, round_up(lon_total // 4, 128)
    f32, bf16 = jnp.float32, jnp.bfloat16
    slab = (col_count, row_count)
    whole = pl.BlockSpec(memory_space=pl.ANY)
    dma = pltpu.SemaphoreType.DMA
    obs = [(table.shape, table.dtype) for table in (obs_level, obs_col, obs_row, obs_value)]
    near = obs + [(seed.shape, f32) for seed in seeds]
    result = pl.pallas_call(
        functools.partial(fused_kernel, lat_size, lon_size, own, obs_row.shape[0]),
        out_shape=jax.ShapeDtypeStruct((level_count,) + slab, bf16),
        in_specs=[whole] * 10,
        out_specs=whole,
        scratch_shapes=[
            pltpu.VMEM((own, lat_size, lon_size) + slab, bf16),
            pltpu.VMEM((2, kind_size, points), bf16),
            pltpu.VMEM((2 * kind_size, 2 * points), bf16),
            pltpu.VMEM((2, points, kind_size), bf16),
            pltpu.VMEM((2 * points, 2 * kind_size), bf16),
            pltpu.VMEM((points, 4 * kind_size), f32),
            pltpu.VMEM((lat_total, lat_total), bf16),
            pltpu.VMEM((part_count, lat_total), f32),
            pltpu.VMEM((4, lat_size, share_pad, lat_total), bf16),
            pltpu.VMEM((half // 2, 3) + obs_row.shape, bf16),
            pltpu.VMEM((half, 3) + obs_row.shape, bf16),
            pltpu.VMEM((3,) + obs_row.shape, f32),
            pltpu.VMEM(slab, f32),
            pltpu.VMEM((half // 2, col_count, 2 * row_count), f32),
            pltpu.VMEM((half // 2,) + slab, bf16),
            pltpu.VMEM((lat_size, lon_size) + slab, bf16),
            pltpu.VMEM((4 * points, 2 * row_count), bf16),
            pltpu.VMEM((4 * kind_size, 2 * row_count), bf16),
            pltpu.VMEM((4 * kind_size, lat_total), f32),
            pltpu.VMEM((4 * kind_size, lat_total), bf16),
            pltpu.VMEM((4 * kind_size, 2 * row_count), bf16),
            pltpu.VMEM((lon_size, lat_size) + slab, f32),
            pltpu.VMEM((half, lat_size) + slab, f32),
            pltpu.VMEM((half // 2, lat_size) + slab, bf16),
            pltpu.VMEM((half // 2, lat_size) + slab, bf16),
            pltpu.VMEM((half // 2, lat_size) + slab, bf16),
            pltpu.VMEM((half, lat_size) + slab, bf16),
            pltpu.VMEM((half // 2,) + slab, bf16),
            pltpu.VMEM((level_count,) + slab, bf16),
            *[pltpu.VMEM(shape, dtype) for shape, dtype in near],
            dma((own, lat_size, lon_size)), dma((own, lat_size, lon_size)), dma((own,)), dma((9,)),
            dma((lat_size,)), dma((lat_size,)), dma((lat_size,)), dma((lat_size,)),
            dma((half // 2,)), dma((half,)), dma((half // 2,)), dma((lon_size,)),
            dma((lat_size,)), dma((lat_size,)), dma((lat_size,)), dma((lat_size,)),
            dma((half, lat_size // 2)), dma((half, lat_size // 2)), dma((half // 2, lat_size, 2)),
            dma((half // 2, lat_size, 2)), dma((half // 2, lat_size)), dma((half, lat_size)),
            dma((half // 2, 2)), dma((lon_size, 2)), dma((lon_size,)), dma((lon_size,)), dma((lon_size,)),
        ],
        compiler_params=pltpu.CompilerParams(
            collective_id=0, has_side_effects=True, vmem_limit_bytes=60 * 1024 * 1024
        ),
    )(
        anomalies, taper, obs_level, obs_col, obs_row, obs_value, *seeds,
    )
    return result.astype(f32) / (ensemble - 1)


def solution(mesh):
    in_specs = (
        P("mem", None, "lon", "lat"),
        P("lon", "lat", None),
        P("lat", "lon"),
        P("lat", "lon"),
        P("lat", "lon"),
        P("lat", "lon"),
    )
    out_specs = P(None, "lon", "lat")
    return jax.shard_map(local, mesh=mesh, in_specs=in_specs, out_specs=out_specs, check_vma=False)
```

```python
import functools
import math

import jax
import jax.numpy as jnp
import numpy as np
from jax import lax
from jax.experimental import pallas as pl
from jax.experimental.pallas import tpu as pltpu
from jax.sharding import PartitionSpec as P


CLASSES = (0, 2, 1, 3)


def round_up(size, unit):
    return -(-size // unit) * unit


def lon_seeds(length, part_count):
    nyquist = length // 2
    quarter = length // 4
    inner = next(n for n in range(24, 0, -8) if quarter % n == 0)
    outer = quarter // inner
    share = quarter // part_count
    padded = round_up(share, 16)
    offsets = np.arange(padded)
    coef_idx = np.stack([
        np.stack([part * (length // part_count) + 4 * offsets + kind for part in range(part_count)])
        for kind in CLASSES
    ])
    real = np.broadcast_to(offsets < share, coef_idx.shape).reshape(-1)
    coef_idx = np.where(real, coef_idx.reshape(-1), 0)
    wavenum = np.where(coef_idx <= nyquist, coef_idx, coef_idx - nyquist)

    def waves(points):
        angles = (points[:, None] * wavenum[None, :] % length) * (2.0 * math.pi / length)
        return np.cos(angles), np.sin(angles)

    scales = np.where((coef_idx == 0) | (coef_idx == nyquist), 1.0 / math.sqrt(length), math.sqrt(2.0 / length))
    scales = np.where(real, scales, 0.0)
    is_cos = coef_idx <= nyquist
    starts = np.arange(2)[:, None] * quarter + np.arange(outer)[None, :] * inner
    high_cos, high_sin = waves(starts.reshape(-1))
    first = np.where(is_cos, high_cos, high_sin) * scales
    second = np.where(is_cos, -high_sin, high_cos) * scales
    high = np.stack([first, second]).reshape(2, 2, outer, -1)
    low = np.stack(waves(np.arange(inner)))
    return [jnp.asarray(part, jnp.float32) for part in (high, low)]


def lat_seeds(length):
    inner = next(size for size in range(32, 0, -1) if length % size == 0)
    outer = length // inner
    mode_idx = np.arange(length)[None, :]

    def waves(points):
        angles = (mode_idx * points[:, None] % (4 * length)) * (math.pi / (2.0 * length))
        return np.cos(angles), np.sin(angles)

    scales = np.where(mode_idx == 0, 1.0 / math.sqrt(length), math.sqrt(2.0 / length))
    high = np.stack(waves(np.arange(outer) * (2 * inner))) * scales
    low = np.stack(waves(np.arange(inner) * 2 + 1))
    return [jnp.asarray(part, jnp.float32) for part in (high, low)]


def fused_kernel(
    lat_size, lon_size, own, obs_rows,
    anom, taper, level, column, row, value, lon_high, lon_low, lat_high, lat_low, out,
    fields, even_fwd, odd_fwd, even_inv, odd_inv, fine, modes, taper_near, taper_all, far_send, far_recv, far_near, far_hits, hits, innov_own, innov_all,
    folded, zonal, spectrum, tapered, inverse, total, partner_part, lat_send, lat_recv, near_send, near_recv, lon_send, lon_recv,
    level_near, column_near, row_near, value_near, high_near, low_near, lat_high_near, lat_low_near,
    field_ss, field_rs, local_sem, table_sem, taper_ss, taper_rs, trade_ss, trade_rs, far_ss, far_rs, innov_ss, innov_rs,
    gather_ss, gather_rs, share_ss, share_rs, mem_ss, mem_rs, lat_ss, lat_rs, near_ss, near_rs, lon_ss, lon_rs, pair_ss, pair_rs, out_sem,
):
    lat, lon, mem = lax.axis_index("lat"), lax.axis_index("lon"), lax.axis_index("mem")
    place_count = lat_size * lon_size
    half = lon_size // 2
    quarter = half // 2
    me = lat * lon_size + lon
    side = lax.div(lon, half)
    receives = lax.div(lax.rem(lon, half), quarter) == mem
    col_count, row_count = fields.shape[3:]
    f32, bf16 = jnp.float32, jnp.bfloat16

    def device(lat_idx, lon_idx, mem_idx):
        return {"lat": lat_idx, "lon": lon_idx, "mem": mem_idx}

    partner = device(lat, lon, 1 - mem)

    def remote(src, dst, send, recv, target):
        return pltpu.make_async_remote_copy(
            src_ref=src, dst_ref=dst, send_sem=send, recv_sem=recv,
            device_id=target, device_id_type=pl.DeviceIdType.MESH,
        )

    def owned(idx, core):
        near = lax.div(idx, quarter)
        return (1 - side + near * (2 * side - 1)) * half + core * quarter + lax.rem(idx, quarter)

    near_copies = [
        pltpu.make_async_copy(src, dst, table_sem.at[idx])
        for idx, (src, dst) in enumerate([
            (level, level_near), (column, column_near), (row, row_near), (value, value_near),
            (taper.at[0], taper_near), (lon_high, high_near), (lon_low, low_near),
            (lat_high, lat_high_near), (lat_low, lat_low_near),
        ])
    ]
    for copy in near_copies:
        copy.start()
    col_start, row_start = lon * col_count, lat * row_count
    for copy in near_copies[:4]:
        copy.wait()

    local_col = column_near[...] - col_start
    pairs = lax.shift_right_logical(local_col, 1).astype(f32).astype(bf16)
    parities = (2 * (row_near[...] - row_start) + lax.bitwise_and(local_col, 1)).astype(f32).astype(bf16)
    for idx in range(quarter):
        far_send[idx, 0] = jnp.where(level_near[...] == owned(idx, mem), value_near[...], 0.0).astype(bf16)
        far_send[idx, 1] = pairs
        far_send[idx, 2] = parities

    barrier = pltpu.get_barrier_semaphore()

    @pl.loop(1, place_count)
    def _(offset):
        spot = lax.rem(me + offset, place_count)
        pl.semaphore_signal(
            barrier, inc=1, device_id=device(lax.div(spot, lon_size), lax.rem(spot, lon_size), mem),
            device_id_type=pl.DeviceIdType.MESH,
        )

    pl.semaphore_signal(barrier, inc=1, device_id=partner, device_id_type=pl.DeviceIdType.MESH)
    pl.semaphore_wait(barrier, place_count)

    def far_copy(idx):
        return remote(
            far_send.at[idx], far_recv.at[lax.rem(lon, half)], far_ss.at[idx], far_rs.at[lax.rem(lon, half)],
            device(lat, owned(idx, mem), mem),
        )

    for idx in range(quarter):
        far_copy(idx).start()

    def field_copy(turn, slot, step):
        lat_idx, lon_idx = lax.rem(lat + slot, lat_size), lax.rem(lon + step, lon_size)
        return remote(
            anom.at[lat_idx * own + turn, lon_idx], fields.at[turn, slot, lon],
            field_ss.at[turn, slot, step], field_rs.at[turn, slot, step], device(lat_idx, lon_idx, mem),
        )

    def send_fields(turn, slot):
        @pl.loop(0, lon_size - 1 if slot == 0 else lon_size)
        def _(idx):
            step = half + lax.div(idx + 1, 2) * (1 - 2 * lax.rem(idx, 2))
            field_copy(turn, slot, step).start()

    def own_copy(turn):
        return pltpu.make_async_copy(
            anom.at[lat * own + turn, lon], fields.at[turn, 0, lon], local_sem.at[turn]
        )

    lead = lat_size // 2
    for slot in range(lead):
        send_fields(0, slot)
    for turn in range(own):
        own_copy(turn).start()

    hits[...] = jnp.zeros_like(hits)
    group = 4

    @pl.loop(0, obs_rows // group)
    def _(step):
        def wide(ref):
            return jnp.concatenate([ref[pl.ds(step * group + part, 1), :] for part in range(group)], axis=1)

        keys = wide(level_near) * col_count + (wide(column_near) - col_start)
        local_row = wide(row_near) - row_start
        amount = wide(value_near)
        width = keys.shape[1]
        high = amount.astype(bf16).astype(f32)
        low = amount - high
        row_hot = lax.broadcasted_iota(jnp.int32, (row_count, width), 0) == local_row
        right = jnp.concatenate(
            [jnp.where(row_hot, high, 0.0).astype(bf16), jnp.where(row_hot, low, 0.0).astype(bf16)], axis=0
        )
        cells = lax.broadcasted_iota(jnp.int32, (col_count, width), 0)
        for idx in range(quarter):
            left = jnp.where(cells == keys - owned(quarter + idx, mem) * col_count, 1.0, 0.0).astype(bf16)
            hits[idx] += lax.dot_general(
                left, right, (((1,), (1,)), ((), ())), preferred_element_type=f32
            )

    def innov_copy(idx):
        lev = owned(quarter + idx, mem)
        return remote(
            innov_own.at[idx], innov_all.at[0, lon], innov_ss.at[idx], innov_rs.at[lon], device(lat, lev, mem)
        )

    for idx in range(quarter):
        block = (hits[idx, :, :row_count] + hits[idx, :, row_count:]).astype(bf16)
        innov_own[idx] = block
        lev = owned(quarter + idx, mem)
        pl.when(lev != lon)(lambda idx=idx: innov_copy(idx).start())

        @pl.when(lev == lon)
        def _(block=block):
            innov_all[0, lon] = block

    for slot in range(lead, lat_size):
        send_fields(0, slot)
    def gather_copy(slot):
        return remote(
            innov_all.at[0], innov_all.at[slot], gather_ss.at[slot], gather_rs.at[slot],
            device(lax.rem(lat + slot, lat_size), lon, mem),
        )

    def share_copy(slot):
        return remote(innov_all.at[slot], innov_all.at[slot], share_ss.at[slot], share_rs.at[slot], partner)

    @pl.when(receives)
    def _():
        @pl.loop(0, half)
        def _(source):
            remote(
                far_send.at[0], far_recv.at[source], far_ss.at[0], far_rs.at[source],
                device(lat, (1 - side) * half + source, mem),
            ).wait_recv()
            far_near[...] = far_recv[source].astype(f32)
            far_hits[...] = jnp.zeros_like(far_hits)

            @pl.loop(0, obs_rows // group)
            def _(step):
                def wide(kind):
                    return jnp.concatenate(
                        [far_near[kind, pl.ds(step * group + part, 1), :] for part in range(group)], axis=1
                    )

                coded = wide(2).astype(jnp.int32)
                local_row = lax.shift_right_logical(coded, 1)
                local_col = 2 * wide(1).astype(jnp.int32) + lax.bitwise_and(coded, 1)
                width = coded.shape[1]
                row_hot = lax.broadcasted_iota(jnp.int32, (row_count, width), 0) == local_row
                right = jnp.where(row_hot, wide(0), 0.0).astype(bf16)
                cells = lax.broadcasted_iota(jnp.int32, (col_count, width), 0)
                left = jnp.where(cells == local_col, 1.0, 0.0).astype(bf16)
                far_hits[...] += lax.dot_general(
                    left, right, (((1,), (1,)), ((), ())), preferred_element_type=f32
                )

            innov_all[0, (1 - side) * half + source] = far_hits[...].astype(bf16)

        for idx in range(1, half):
            sender = side * half + lax.rem(lon + idx, half)
            remote(
                innov_own.at[0], innov_all.at[0, sender], innov_ss.at[0], innov_rs.at[sender],
                device(lat, sender, mem),
            ).wait_recv()
        for slot in range(1, lat_size):
            gather_copy(slot).start()
        share_copy(0).start()

    near_copies[4].wait()
    share, share_pad = taper_near.shape[0] // 4, taper_all.shape[2]
    modes_half = taper_near.shape[1] // 2
    spread = (4 * share_pad, 4 * share)
    out_row = lax.broadcasted_iota(jnp.int32, spread, 0)
    in_row = lax.broadcasted_iota(jnp.int32, spread, 1)
    chosen = jnp.zeros(spread, jnp.bool_)
    for idx, kind in enumerate(CLASSES):
        local_row = out_row - idx * share_pad
        chosen |= (local_row >= 0) & (local_row < share) & (in_row == 4 * local_row + kind)
    by_class = jnp.dot(
        jnp.where(chosen, 1.0, 0.0).astype(bf16), taper_near[...].astype(bf16), preferred_element_type=f32
    ).astype(bf16)
    for idx in range(4):
        taper_all[idx, lat] = by_class[idx * share_pad:(idx + 1) * share_pad]
    lanes = pl.ds(pl.multiple_of(mem * modes_half, modes_half), modes_half)

    def taper_copy(step):
        part = taper_all.at[:, lat, :, lanes]
        return remote(
            part, part, taper_ss.at[step], taper_rs.at[step], device(lax.rem(lat + step, lat_size), lon, mem)
        )

    def trade_copy(step):
        part = taper_all.at[:, lax.rem(lat + lat_size - step, lat_size), :, lanes]
        return remote(part, part, trade_ss.at[step], trade_rs.at[step], partner)

    for step in range(1, lat_size):
        taper_copy(step).start()

    for turn in range(1, own - 1):
        for slot in range(lat_size):
            send_fields(turn, slot)

    @pl.loop(0, lon_size)
    def _(idx):
        step = half + lax.div(idx + 1, 2) * (1 - 2 * lax.rem(idx, 2))
        for slot in range(lat_size):
            pl.when(slot + step > 0)(lambda slot=slot: field_copy(own - 1, slot, step).start())

    for copy in near_copies[5:]:
        copy.wait()

    outer, inner = high_near.shape[2], low_near.shape[1]
    points, kind_size = even_inv.shape[1:]
    span = outer * inner
    low_cos, low_sin = low_near[0], low_near[1]
    fine[span:, :] = jnp.zeros((points - span, 4 * kind_size), f32)
    for block in range(2):
        first = 2 * block * kind_size
        for idx in range(outer):
            fine[idx * inner:(idx + 1) * inner, first:] = (
                high_near[0, block, idx:idx + 1, first:] * low_cos[:, first:]
                + high_near[1, block, idx:idx + 1, first:] * low_sin[:, first:]
            )
        for kind in range(2 * block, 4):
            tile = fine[:, kind * kind_size:(kind + 1) * kind_size]
            if kind < 2:
                even_inv[kind] = tile.astype(bf16)
                even_fwd[kind] = tile.T.astype(bf16)
            else:
                rows = slice(block * points, (block + 1) * points)
                cols = slice((kind - 2) * kind_size, (kind - 1) * kind_size)
                odd_inv[rows, cols] = tile.astype(bf16)
                odd_fwd[cols, rows] = tile.T.astype(bf16)
    folded[...] = jnp.zeros_like(folded)

    lat_inner = lat_low_near.shape[1]
    per_band = row_count // lat_inner
    lat_cos, lat_sin = lat_low_near[0], lat_low_near[1]
    for slot in range(lat_size):
        band = lax.rem(lat + lat_size - slot, lat_size)
        for idx in range(per_band):
            spot = pl.ds(band * per_band + idx, 1)
            rows = slice(slot * row_count + idx * lat_inner, slot * row_count + (idx + 1) * lat_inner)
            modes[rows, :] = (
                lat_high_near[0, spot, :] * lat_cos - lat_high_near[1, spot, :] * lat_sin
            ).astype(bf16)

    @pl.when(receives)
    def _():
        for slot in range(1, lat_size):
            gather_copy(slot).wait_recv()
            share_copy(slot).start()

    @pl.when(jnp.logical_not(receives))
    def _():
        for slot in range(lat_size):
            share_copy(slot).wait_recv()

    total[...] = jnp.zeros_like(total)
    for step in range(1, lat_size):
        taper_copy(step).wait_recv()
        trade_copy(step).start()
    for step in range(1, lat_size):
        trade_copy(step).wait_recv()

    stages = lat_size // 2
    pair = 2 * row_count
    fourth = lon_size // 4
    kinds = 4 * kind_size

    def fold(turn, slot, lanes):
        def quarter_of(which):
            parts = []
            for idx in range(fourth):
                block = which * fourth + idx
                parts.append(fields[turn, slot, block].astype(f32) * innov_all[slot, block].astype(f32))
            return parts[0] if fourth == 1 else jnp.concatenate(parts, axis=0)

        first, second, third, last = [quarter_of(which) for which in range(4)]
        even, odd = first + third, second + last
        for idx, value in enumerate([even + odd, even - odd, first - third, second - last]):
            folded[pl.ds(idx * points, span), lanes] = value.astype(bf16)

    def zonal_of(turn, stage):
        for which in range(2):
            slot = 2 * stage + which

            @pl.loop(0, lon_size)
            def _(step, slot=slot):
                pl.when(slot + step == 0)(lambda: own_copy(turn).wait())
                pl.when(slot + step > 0)(lambda: field_copy(turn, slot, step).wait_recv())

            fold(turn, slot, slice(which * row_count, (which + 1) * row_count))
        for kind in range(2):
            zonal[kind * kind_size:(kind + 1) * kind_size, :] = jnp.dot(
                even_fwd[kind], folded[kind * points:(kind + 1) * points, :], preferred_element_type=f32
            ).astype(bf16)
        zonal[2 * kind_size:, :] = jnp.dot(
            odd_fwd[...], folded[2 * points:, :], preferred_element_type=f32
        ).astype(bf16)
        return jnp.dot(zonal[...], modes[stage * pair:(stage + 1) * pair, :], preferred_element_type=f32)

    def transform(turn):
        for stage in range(stages - 1):
            terms = zonal_of(turn, stage)
            spectrum[...] = terms if stage == 0 else spectrum[...] + terms
        terms = zonal_of(turn, stages - 1) + spectrum[...]
        tapered[...] = (terms * taper_all[...].reshape(kinds, lat_size * row_count).astype(f32)).astype(bf16)

    def localize(turn, stage):
        inverse[...] = lax.dot_general(
            tapered[...], modes[pl.ds(pl.multiple_of(stage * pair, pair), pair), :],
            (((1,), (1,)), ((), ())), preferred_element_type=f32,
        ).astype(bf16)

        def back(table, rows):
            return jnp.dot(table, inverse[rows, :], preferred_element_type=f32)

        even = back(even_inv[0, :span], slice(0, kind_size))
        swing = back(even_inv[1, :span], slice(kind_size, 2 * kind_size))
        odd = [back(odd_inv[idx * points:idx * points + span, :], slice(2 * kind_size, kinds)) for idx in range(2)]
        for which in range(4):
            base = even + swing if which % 2 == 0 else even - swing
            values = base + odd[which % 2] if which < 2 else base - odd[which % 2]
            for idx in range(fourth):
                block = which * fourth + idx
                for part in range(2):
                    slot = 2 * stage + part
                    total[block, slot] += (
                        fields[turn, slot, block].astype(f32)
                        * values[idx * col_count:(idx + 1) * col_count, part * row_count:(part + 1) * row_count]
                    )

    @pl.loop(0, own - 1)
    def _(turn):
        transform(turn)
        pl.loop(0, stages)(lambda stage: localize(turn, stage))

    transform(own - 1)

    def mem_copy(idx, stage):
        slots = pl.ds(2 * stage, 2)
        return remote(
            total.at[owned(idx, 1 - mem), slots], partner_part.at[idx, slots],
            mem_ss.at[idx, stage], mem_rs.at[idx, stage], partner,
        )

    @pl.loop(0, stages)
    def _(step):
        stage = stages - 1 - step
        localize(own - 1, stage)
        for idx in range(half):
            mem_copy(idx, stage).start()

    cutoff = col_count // 2 // 16 * 16
    bands = [slice(0, cutoff), slice(cutoff, col_count)]

    def lat_copy(idx, slot, band):
        rows = bands[band]
        return remote(
            lat_send.at[idx, slot, rows], lat_recv.at[idx, slot, rows],
            lat_ss.at[idx, slot, band], lat_rs.at[idx, slot, band],
            device(lax.rem(lat + lat_size - slot, lat_size), lon, mem),
        )

    def near_copy(idx, slot):
        return remote(
            near_send.at[idx, slot], near_recv.at[lax.rem(lon, half), slot],
            near_ss.at[idx, slot], near_rs.at[lax.rem(lon, half), slot],
            device(lax.rem(lat + lat_size - slot, lat_size), owned(quarter + idx, mem), mem),
        )

    slots = range(lat_size - 1, -1, -1)
    for idx in range(quarter):
        block = owned(idx, mem)
        for band in range(2):
            for slot in slots:
                if band == 0 and slot % 2 == 1:
                    mem_copy(idx, slot // 2).wait_recv()
                rows = bands[band]
                lat_send[idx, slot, rows] = (total[block, slot, rows] + partner_part[idx, slot, rows]).astype(bf16)
                if slot > 0:
                    lat_copy(idx, slot, band).start()
    for idx in range(quarter):
        block = owned(quarter + idx, mem)
        for slot in slots:
            if slot % 2 == 1:
                mem_copy(quarter + idx, slot // 2).wait_recv()
            value = (total[block, slot] + partner_part[quarter + idx, slot]).astype(bf16)
            if slot > 0:
                near_send[idx, slot] = value
                near_copy(idx, slot).start()
            else:
                @pl.when(block != lon)
                def _(idx=idx, value=value):
                    near_send[idx, 0] = value
                    near_copy(idx, 0).start()

                @pl.when(block == lon)
                def _(value=value):
                    near_recv[lax.rem(lon, half), 0] = value

    def lon_copy(idx, band):
        rows = bands[band]
        return remote(
            lon_send.at[idx, rows], lon_recv.at[lon, rows], lon_ss.at[idx, band], lon_rs.at[lon, band],
            device(lat, owned(idx, mem), mem),
        )

    for band in range(2):
        rows = bands[band]
        for idx in range(quarter):
            summed = lat_send[idx, 0, rows].astype(f32)
            for slot in range(1, lat_size):
                lat_copy(idx, slot, band).wait_recv()
                summed += lat_recv[idx, slot, rows].astype(f32)
            lon_send[idx, rows] = summed.astype(bf16)
            lon_copy(idx, band).start()

    def pair_copy(sender):
        return remote(lon_recv.at[sender], out.at[sender], pair_ss.at[sender], pair_rs.at[sender], partner)

    def out_copy(sender):
        return pltpu.make_async_copy(lon_recv.at[sender], out.at[sender], out_sem.at[sender])

    far = [(1 - side) * half + idx for idx in range(half)]
    close = [side * half + lax.rem(lon + idx, half) for idx in range(half)]

    @pl.when(receives)
    def _():
        for idx, sender in enumerate(close):
            local_level = lax.rem(lon + idx, half)
            summed = None
            for slot in range(lat_size):
                if idx + slot > 0:
                    remote(
                        near_send.at[0, slot], near_recv.at[local_level, slot], near_ss.at[0, slot],
                        near_rs.at[local_level, slot], device(lax.rem(lat + slot, lat_size), sender, mem),
                    ).wait_recv()
                term = near_recv[local_level, slot].astype(f32)
                summed = term if slot == 0 else summed + term
            lon_recv[sender] = summed.astype(bf16)
            pair_copy(sender).start()
            out_copy(sender).start()
        for sender in far:
            for band in range(2):
                rows = bands[band]
                remote(
                    lon_send.at[0, rows], lon_recv.at[sender, rows], lon_ss.at[0, band], lon_rs.at[sender, band],
                    device(lat, sender, mem),
                ).wait_recv()
            pair_copy(sender).start()
            out_copy(sender).start()

    @pl.when(jnp.logical_not(receives))
    def _():
        for sender in close + far:
            pair_copy(sender).wait_recv()

    @pl.when(receives)
    def _():
        for sender in close + far:
            pair_copy(sender).wait_send()
            out_copy(sender).wait()
        for slot in range(1, lat_size):
            gather_copy(slot).wait_send()
        for slot in range(lat_size):
            share_copy(slot).wait_send()

    for idx in range(half):
        for stage in range(stages):
            mem_copy(idx, stage).wait_send()
    for idx in range(quarter):
        for band in range(2):
            lon_copy(idx, band).wait_send()
            for slot in range(1, lat_size):
                lat_copy(idx, slot, band).wait_send()
        for slot in range(1, lat_size):
            near_copy(idx, slot).wait_send()
        pl.when(owned(quarter + idx, mem) != lon)(lambda idx=idx: near_copy(idx, 0).wait_send())
        pl.when(owned(quarter + idx, mem) != lon)(lambda idx=idx: innov_copy(idx).wait_send())
        far_copy(idx).wait_send()
    for step in range(1, lat_size):
        taper_copy(step).wait_send()
        trade_copy(step).wait_send()

    @pl.loop(0, own)
    def _(turn):
        for slot in range(lat_size):
            @pl.loop(1 if slot == 0 else 0, lon_size)
            def _(step, slot=slot):
                field_copy(turn, slot, step).wait_send()


def local(anomalies, taper, obs_row, obs_col, obs_level, obs_value):
    member_count, level_count, col_count, row_count = anomalies.shape
    lon_size, lat_size = lax.axis_size("lon"), lax.axis_size("lat")
    lat_total = row_count * lat_size
    ensemble = member_count * lax.axis_size("mem")
    own = member_count // lat_size
    half = lon_size // 2
    part_count = taper.shape[1]
    lon_total = col_count * lon_size
    seeds = lon_seeds(lon_total, lat_size) + lat_seeds(lat_total)
    share_pad = round_up(part_count // 4, 16)
    kind_size, points = lat_size * share_pad, round_up(lon_total // 4, 128)
    f32, bf16 = jnp.float32, jnp.bfloat16
    slab = (col_count, row_count)
    whole = pl.BlockSpec(memory_space=pl.ANY)
    dma = pltpu.SemaphoreType.DMA
    obs = [(table.shape, table.dtype) for table in (obs_level, obs_col, obs_row, obs_value)]
    near = obs + [(seed.shape, f32) for seed in seeds]
    result = pl.pallas_call(
        functools.partial(fused_kernel, lat_size, lon_size, own, obs_row.shape[0]),
        out_shape=jax.ShapeDtypeStruct((level_count,) + slab, bf16),
        in_specs=[whole] * 10,
        out_specs=whole,
        scratch_shapes=[
            pltpu.VMEM((own, lat_size, lon_size) + slab, bf16),
            pltpu.VMEM((2, kind_size, points), bf16),
            pltpu.VMEM((2 * kind_size, 2 * points), bf16),
            pltpu.VMEM((2, points, kind_size), bf16),
            pltpu.VMEM((2 * points, 2 * kind_size), bf16),
            pltpu.VMEM((points, 4 * kind_size), f32),
            pltpu.VMEM((lat_total, lat_total), bf16),
            pltpu.VMEM((part_count, lat_total), f32),
            pltpu.VMEM((4, lat_size, share_pad, lat_total), bf16),
            pltpu.VMEM((half // 2, 3) + obs_row.shape, bf16),
            pltpu.VMEM((half, 3) + obs_row.shape, bf16),
            pltpu.VMEM((3,) + obs_row.shape, f32),
            pltpu.VMEM(slab, f32),
            pltpu.VMEM((half // 2, col_count, 2 * row_count), f32),
            pltpu.VMEM((half // 2,) + slab, bf16),
            pltpu.VMEM((lat_size, lon_size) + slab, bf16),
            pltpu.VMEM((4 * points, 2 * row_count), bf16),
            pltpu.VMEM((4 * kind_size, 2 * row_count), bf16),
            pltpu.VMEM((4 * kind_size, lat_total), f32),
            pltpu.VMEM((4 * kind_size, lat_total), bf16),
            pltpu.VMEM((4 * kind_size, 2 * row_count), bf16),
            pltpu.VMEM((lon_size, lat_size) + slab, f32),
            pltpu.VMEM((half, lat_size) + slab, f32),
            pltpu.VMEM((half // 2, lat_size) + slab, bf16),
            pltpu.VMEM((half // 2, lat_size) + slab, bf16),
            pltpu.VMEM((half // 2, lat_size) + slab, bf16),
            pltpu.VMEM((half, lat_size) + slab, bf16),
            pltpu.VMEM((half // 2,) + slab, bf16),
            pltpu.VMEM((level_count,) + slab, bf16),
            *[pltpu.VMEM(shape, dtype) for shape, dtype in near],
            dma((own, lat_size, lon_size)), dma((own, lat_size, lon_size)), dma((own,)), dma((9,)),
            dma((lat_size,)), dma((lat_size,)), dma((lat_size,)), dma((lat_size,)),
            dma((half // 2,)), dma((half,)), dma((half // 2,)), dma((lon_size,)),
            dma((lat_size,)), dma((lat_size,)), dma((lat_size,)), dma((lat_size,)),
            dma((half, lat_size // 2)), dma((half, lat_size // 2)), dma((half // 2, lat_size, 2)),
            dma((half // 2, lat_size, 2)), dma((half // 2, lat_size)), dma((half, lat_size)),
            dma((half // 2, 2)), dma((lon_size, 2)), dma((lon_size,)), dma((lon_size,)), dma((lon_size,)),
        ],
        compiler_params=pltpu.CompilerParams(
            collective_id=0, has_side_effects=True, vmem_limit_bytes=60 * 1024 * 1024
        ),
    )(
        anomalies, taper, obs_level, obs_col, obs_row, obs_value, *seeds,
    )
    return result.astype(f32) / (ensemble - 1)


def solution(mesh):
    in_specs = (
        P("mem", None, "lon", "lat"),
        P("lon", "lat", None),
        P("lat", "lon"),
        P("lat", "lon"),
        P("lat", "lon"),
        P("lat", "lon"),
    )
    out_specs = P(None, "lon", "lat")
    return jax.shard_map(local, mesh=mesh, in_specs=in_specs, out_specs=out_specs, check_vma=False)
```

```python
import functools
import math

import jax
import jax.numpy as jnp
import numpy as np
from jax import lax
from jax.experimental import pallas as pl
from jax.experimental.pallas import tpu as pltpu
from jax.sharding import PartitionSpec as P


CLASSES = (0, 2, 1, 3)


def round_up(size, unit):
    return -(-size // unit) * unit


def lon_seeds(length, part_count):
    nyquist = length // 2
    quarter = length // 4
    inner = next(n for n in range(24, 0, -8) if quarter % n == 0)
    outer = quarter // inner
    share = quarter // part_count
    padded = round_up(share, 16)
    offsets = np.arange(padded)
    coef_idx = np.stack([
        np.stack([part * (length // part_count) + 4 * offsets + kind for part in range(part_count)])
        for kind in CLASSES
    ])
    real = np.broadcast_to(offsets < share, coef_idx.shape).reshape(-1)
    coef_idx = np.where(real, coef_idx.reshape(-1), 0)
    wavenum = np.where(coef_idx <= nyquist, coef_idx, coef_idx - nyquist)

    def waves(points):
        angles = (points[:, None] * wavenum[None, :] % length) * (2.0 * math.pi / length)
        return np.cos(angles), np.sin(angles)

    scales = np.where((coef_idx == 0) | (coef_idx == nyquist), 1.0 / math.sqrt(length), math.sqrt(2.0 / length))
    scales = np.where(real, scales, 0.0)
    is_cos = coef_idx <= nyquist
    starts = np.arange(2)[:, None] * quarter + np.arange(outer)[None, :] * inner
    high_cos, high_sin = waves(starts.reshape(-1))
    first = np.where(is_cos, high_cos, high_sin) * scales
    second = np.where(is_cos, -high_sin, high_cos) * scales
    high = np.stack([first, second]).reshape(2, 2, outer, -1)
    low = np.stack(waves(np.arange(inner)))
    return [jnp.asarray(part, jnp.float32) for part in (high, low)]


def lat_seeds(length):
    inner = next(size for size in range(32, 0, -1) if length % size == 0)
    outer = length // inner
    mode_idx = np.arange(length)[None, :]

    def waves(points):
        angles = (mode_idx * points[:, None] % (4 * length)) * (math.pi / (2.0 * length))
        return np.cos(angles), np.sin(angles)

    scales = np.where(mode_idx == 0, 1.0 / math.sqrt(length), math.sqrt(2.0 / length))
    high = np.stack(waves(np.arange(outer) * (2 * inner))) * scales
    low = np.stack(waves(np.arange(inner) * 2 + 1))
    return [jnp.asarray(part, jnp.float32) for part in (high, low)]


def fused_kernel(
    lat_size, lon_size, own, obs_rows,
    anom, taper, level, column, row, value, lon_high, lon_low, lat_high, lat_low, out,
    fields, even_fwd, odd_fwd, even_inv, odd_inv, fine, modes, taper_near, taper_all, far_send, far_recv, far_near, far_hits, hits, innov_own, innov_all,
    folded, zonal, spectrum, tapered, inverse, total, partner_part, lat_send, lat_recv, near_send, near_recv, lon_send, lon_recv,
    level_near, column_near, row_near, value_near, high_near, low_near, lat_high_near, lat_low_near,
    field_ss, field_rs, local_sem, table_sem, taper_ss, taper_rs, trade_ss, trade_rs, far_ss, far_rs, innov_ss, innov_rs,
    gather_ss, gather_rs, share_ss, share_rs, mem_ss, mem_rs, lat_ss, lat_rs, near_ss, near_rs, lon_ss, lon_rs, pair_ss, pair_rs, out_sem,
):
    lat, lon, mem = lax.axis_index("lat"), lax.axis_index("lon"), lax.axis_index("mem")
    place_count = lat_size * lon_size
    half = lon_size // 2
    quarter = half // 2
    me = lat * lon_size + lon
    side = lax.div(lon, half)
    receives = lax.div(lax.rem(lon, half), quarter) == mem
    col_count, row_count = fields.shape[3:]
    f32, bf16 = jnp.float32, jnp.bfloat16

    def device(lat_idx, lon_idx, mem_idx):
        return {"lat": lat_idx, "lon": lon_idx, "mem": mem_idx}

    partner = device(lat, lon, 1 - mem)

    def remote(src, dst, send, recv, target):
        return pltpu.make_async_remote_copy(
            src_ref=src, dst_ref=dst, send_sem=send, recv_sem=recv,
            device_id=target, device_id_type=pl.DeviceIdType.MESH,
        )

    def owned(idx, core):
        near = lax.div(idx, quarter)
        return (1 - side + near * (2 * side - 1)) * half + core * quarter + lax.rem(idx, quarter)

    near_copies = [
        pltpu.make_async_copy(src, dst, table_sem.at[idx])
        for idx, (src, dst) in enumerate([
            (level, level_near), (column, column_near), (row, row_near), (value, value_near),
            (taper.at[0], taper_near), (lon_high, high_near), (lon_low, low_near),
            (lat_high, lat_high_near), (lat_low, lat_low_near),
        ])
    ]
    for copy in near_copies:
        copy.start()
    col_start, row_start = lon * col_count, lat * row_count
    for copy in near_copies[:4]:
        copy.wait()

    local_col = column_near[...] - col_start
    pairs = lax.shift_right_logical(local_col, 1).astype(f32).astype(bf16)
    parities = (2 * (row_near[...] - row_start) + lax.bitwise_and(local_col, 1)).astype(f32).astype(bf16)
    for idx in range(quarter):
        far_send[idx, 0] = jnp.where(level_near[...] == owned(idx, mem), value_near[...], 0.0).astype(bf16)
        far_send[idx, 1] = pairs
        far_send[idx, 2] = parities

    barrier = pltpu.get_barrier_semaphore()

    @pl.loop(1, place_count)
    def _(offset):
        spot = lax.rem(me + offset, place_count)
        pl.semaphore_signal(
            barrier, inc=1, device_id=device(lax.div(spot, lon_size), lax.rem(spot, lon_size), mem),
            device_id_type=pl.DeviceIdType.MESH,
        )

    pl.semaphore_signal(barrier, inc=1, device_id=partner, device_id_type=pl.DeviceIdType.MESH)
    pl.semaphore_wait(barrier, place_count)

    def far_copy(idx):
        return remote(
            far_send.at[idx], far_recv.at[lax.rem(lon, half)], far_ss.at[idx], far_rs.at[lax.rem(lon, half)],
            device(lat, owned(idx, mem), mem),
        )

    for idx in range(quarter):
        far_copy(idx).start()

    def field_copy(turn, slot, step):
        lat_idx, lon_idx = lax.rem(lat + slot, lat_size), lax.rem(lon + step, lon_size)
        return remote(
            anom.at[lat_idx * own + turn, lon_idx], fields.at[turn, slot, lon],
            field_ss.at[turn, slot, step], field_rs.at[turn, slot, step], device(lat_idx, lon_idx, mem),
        )

    def send_fields(turn, slot):
        @pl.loop(0, lon_size - 1 if slot == 0 else lon_size)
        def _(idx):
            step = half + lax.div(idx + 1, 2) * (1 - 2 * lax.rem(idx, 2))
            field_copy(turn, slot, step).start()

    def own_copy(turn):
        return pltpu.make_async_copy(
            anom.at[lat * own + turn, lon], fields.at[turn, 0, lon], local_sem.at[turn]
        )

    lead = lat_size // 2
    for slot in range(lead):
        send_fields(0, slot)
    for turn in range(own):
        own_copy(turn).start()

    hits[...] = jnp.zeros_like(hits)
    group = 4

    @pl.loop(0, obs_rows // group)
    def _(step):
        def wide(ref):
            return jnp.concatenate([ref[pl.ds(step * group + part, 1), :] for part in range(group)], axis=1)

        keys = wide(level_near) * col_count + (wide(column_near) - col_start)
        local_row = wide(row_near) - row_start
        amount = wide(value_near)
        width = keys.shape[1]
        high = amount.astype(bf16).astype(f32)
        low = amount - high
        row_hot = lax.broadcasted_iota(jnp.int32, (row_count, width), 0) == local_row
        right = jnp.concatenate(
            [jnp.where(row_hot, high, 0.0).astype(bf16), jnp.where(row_hot, low, 0.0).astype(bf16)], axis=0
        )
        cells = lax.broadcasted_iota(jnp.int32, (col_count, width), 0)
        for idx in range(quarter):
            left = jnp.where(cells == keys - owned(quarter + idx, mem) * col_count, 1.0, 0.0).astype(bf16)
            hits[idx] += lax.dot_general(
                left, right, (((1,), (1,)), ((), ())), preferred_element_type=f32
            )

    def innov_copy(idx):
        lev = owned(quarter + idx, mem)
        return remote(
            innov_own.at[idx], innov_all.at[0, lon], innov_ss.at[idx], innov_rs.at[lon], device(lat, lev, mem)
        )

    for idx in range(quarter):
        block = (hits[idx, :, :row_count] + hits[idx, :, row_count:]).astype(bf16)
        innov_own[idx] = block
        lev = owned(quarter + idx, mem)
        pl.when(lev != lon)(lambda idx=idx: innov_copy(idx).start())

        @pl.when(lev == lon)
        def _(block=block):
            innov_all[0, lon] = block

    for slot in range(lead, lat_size):
        send_fields(0, slot)
    def gather_copy(slot):
        return remote(
            innov_all.at[0], innov_all.at[slot], gather_ss.at[slot], gather_rs.at[slot],
            device(lax.rem(lat + slot, lat_size), lon, mem),
        )

    def share_copy(slot):
        return remote(innov_all.at[slot], innov_all.at[slot], share_ss.at[slot], share_rs.at[slot], partner)

    @pl.when(receives)
    def _():
        @pl.loop(0, half)
        def _(source):
            remote(
                far_send.at[0], far_recv.at[source], far_ss.at[0], far_rs.at[source],
                device(lat, (1 - side) * half + source, mem),
            ).wait_recv()
            far_near[...] = far_recv[source].astype(f32)
            far_hits[...] = jnp.zeros_like(far_hits)

            @pl.loop(0, obs_rows // group)
            def _(step):
                def wide(kind):
                    return jnp.concatenate(
                        [far_near[kind, pl.ds(step * group + part, 1), :] for part in range(group)], axis=1
                    )

                coded = wide(2).astype(jnp.int32)
                local_row = lax.shift_right_logical(coded, 1)
                local_col = 2 * wide(1).astype(jnp.int32) + lax.bitwise_and(coded, 1)
                width = coded.shape[1]
                row_hot = lax.broadcasted_iota(jnp.int32, (row_count, width), 0) == local_row
                right = jnp.where(row_hot, wide(0), 0.0).astype(bf16)
                cells = lax.broadcasted_iota(jnp.int32, (col_count, width), 0)
                left = jnp.where(cells == local_col, 1.0, 0.0).astype(bf16)
                far_hits[...] += lax.dot_general(
                    left, right, (((1,), (1,)), ((), ())), preferred_element_type=f32
                )

            innov_all[0, (1 - side) * half + source] = far_hits[...].astype(bf16)

        for idx in range(1, half):
            sender = side * half + lax.rem(lon + idx, half)
            remote(
                innov_own.at[0], innov_all.at[0, sender], innov_ss.at[0], innov_rs.at[sender],
                device(lat, sender, mem),
            ).wait_recv()
        for slot in range(1, lat_size):
            gather_copy(slot).start()
        share_copy(0).start()

    near_copies[4].wait()
    share, share_pad = taper_near.shape[0] // 4, taper_all.shape[2]
    modes_half = taper_near.shape[1] // 2
    spread = (4 * share_pad, 4 * share)
    out_row = lax.broadcasted_iota(jnp.int32, spread, 0)
    in_row = lax.broadcasted_iota(jnp.int32, spread, 1)
    chosen = jnp.zeros(spread, jnp.bool_)
    for idx, kind in enumerate(CLASSES):
        local_row = out_row - idx * share_pad
        chosen |= (local_row >= 0) & (local_row < share) & (in_row == 4 * local_row + kind)
    by_class = jnp.dot(
        jnp.where(chosen, 1.0, 0.0).astype(bf16), taper_near[...].astype(bf16), preferred_element_type=f32
    ).astype(bf16)
    for idx in range(4):
        taper_all[idx, lat] = by_class[idx * share_pad:(idx + 1) * share_pad]
    lanes = pl.ds(pl.multiple_of(mem * modes_half, modes_half), modes_half)

    def taper_copy(step):
        part = taper_all.at[:, lat, :, lanes]
        return remote(
            part, part, taper_ss.at[step], taper_rs.at[step], device(lax.rem(lat + step, lat_size), lon, mem)
        )

    def trade_copy(step):
        part = taper_all.at[:, lax.rem(lat + lat_size - step, lat_size), :, lanes]
        return remote(part, part, trade_ss.at[step], trade_rs.at[step], partner)

    for step in range(1, lat_size):
        taper_copy(step).start()

    for turn in range(1, own - 1):
        for slot in range(lat_size):
            send_fields(turn, slot)

    @pl.loop(0, lon_size)
    def _(idx):
        step = half + lax.div(idx + 1, 2) * (1 - 2 * lax.rem(idx, 2))
        for slot in range(lat_size):
            pl.when(slot + step > 0)(lambda slot=slot: field_copy(own - 1, slot, step).start())

    for copy in near_copies[5:]:
        copy.wait()

    outer, inner = high_near.shape[2], low_near.shape[1]
    points, kind_size = even_inv.shape[1:]
    span = outer * inner
    low_cos, low_sin = low_near[0], low_near[1]
    fine[span:, :] = jnp.zeros((points - span, 4 * kind_size), f32)
    for block in range(2):
        first = 2 * block * kind_size
        for idx in range(outer):
            fine[idx * inner:(idx + 1) * inner, first:] = (
                high_near[0, block, idx:idx + 1, first:] * low_cos[:, first:]
                + high_near[1, block, idx:idx + 1, first:] * low_sin[:, first:]
            )
        for kind in range(2 * block, 4):
            tile = fine[:, kind * kind_size:(kind + 1) * kind_size]
            if kind < 2:
                even_inv[kind] = tile.astype(bf16)
                even_fwd[kind] = tile.T.astype(bf16)
            else:
                rows = slice(block * points, (block + 1) * points)
                cols = slice((kind - 2) * kind_size, (kind - 1) * kind_size)
                odd_inv[rows, cols] = tile.astype(bf16)
                odd_fwd[cols, rows] = tile.T.astype(bf16)
    folded[...] = jnp.zeros_like(folded)

    lat_inner = lat_low_near.shape[1]
    per_band = row_count // lat_inner
    lat_cos, lat_sin = lat_low_near[0], lat_low_near[1]
    for slot in range(lat_size):
        band = lax.rem(lat + lat_size - slot, lat_size)
        for idx in range(per_band):
            spot = pl.ds(band * per_band + idx, 1)
            rows = slice(slot * row_count + idx * lat_inner, slot * row_count + (idx + 1) * lat_inner)
            modes[rows, :] = (
                lat_high_near[0, spot, :] * lat_cos - lat_high_near[1, spot, :] * lat_sin
            ).astype(bf16)

    @pl.when(receives)
    def _():
        for slot in range(1, lat_size):
            gather_copy(slot).wait_recv()
            share_copy(slot).start()

    @pl.when(jnp.logical_not(receives))
    def _():
        for slot in range(lat_size):
            share_copy(slot).wait_recv()

    total[...] = jnp.zeros_like(total)
    for step in range(1, lat_size):
        taper_copy(step).wait_recv()
        trade_copy(step).start()
    for step in range(1, lat_size):
        trade_copy(step).wait_recv()

    stages = lat_size // 2
    pair = 2 * row_count
    fourth = lon_size // 4
    kinds = 4 * kind_size

    def fold(turn, slot, lanes):
        def quarter_of(which):
            parts = []
            for idx in range(fourth):
                block = which * fourth + idx
                parts.append(fields[turn, slot, block].astype(f32) * innov_all[slot, block].astype(f32))
            return parts[0] if fourth == 1 else jnp.concatenate(parts, axis=0)

        first, second, third, last = [quarter_of(which) for which in range(4)]
        even, odd = first + third, second + last
        for idx, value in enumerate([even + odd, even - odd, first - third, second - last]):
            folded[pl.ds(idx * points, span), lanes] = value.astype(bf16)

    def zonal_of(turn, stage):
        for which in range(2):
            slot = 2 * stage + which

            @pl.loop(0, lon_size)
            def _(step, slot=slot):
                pl.when(slot + step == 0)(lambda: own_copy(turn).wait())
                pl.when(slot + step > 0)(lambda: field_copy(turn, slot, step).wait_recv())

            fold(turn, slot, slice(which * row_count, (which + 1) * row_count))
        for kind in range(2):
            zonal[kind * kind_size:(kind + 1) * kind_size, :] = jnp.dot(
                even_fwd[kind], folded[kind * points:(kind + 1) * points, :], preferred_element_type=f32
            ).astype(bf16)
        zonal[2 * kind_size:, :] = jnp.dot(
            odd_fwd[...], folded[2 * points:, :], preferred_element_type=f32
        ).astype(bf16)
        return jnp.dot(zonal[...], modes[stage * pair:(stage + 1) * pair, :], preferred_element_type=f32)

    def transform(turn):
        for stage in range(stages - 1):
            terms = zonal_of(turn, stage)
            spectrum[...] = terms if stage == 0 else spectrum[...] + terms
        terms = zonal_of(turn, stages - 1) + spectrum[...]
        tapered[...] = (terms * taper_all[...].reshape(kinds, lat_size * row_count).astype(f32)).astype(bf16)

    def localize(turn, stage):
        inverse[...] = lax.dot_general(
            tapered[...], modes[pl.ds(pl.multiple_of(stage * pair, pair), pair), :],
            (((1,), (1,)), ((), ())), preferred_element_type=f32,
        ).astype(bf16)

        def back(table, rows):
            return jnp.dot(table, inverse[rows, :], preferred_element_type=f32)

        even = back(even_inv[0, :span], slice(0, kind_size))
        swing = back(even_inv[1, :span], slice(kind_size, 2 * kind_size))
        odd = [back(odd_inv[idx * points:idx * points + span, :], slice(2 * kind_size, kinds)) for idx in range(2)]
        for which in range(4):
            base = even + swing if which % 2 == 0 else even - swing
            values = base + odd[which % 2] if which < 2 else base - odd[which % 2]
            for idx in range(fourth):
                block = which * fourth + idx
                for part in range(2):
                    slot = 2 * stage + part
                    total[block, slot] += (
                        fields[turn, slot, block].astype(f32)
                        * values[idx * col_count:(idx + 1) * col_count, part * row_count:(part + 1) * row_count]
                    )

    @pl.loop(0, own - 1)
    def _(turn):
        transform(turn)
        pl.loop(0, stages)(lambda stage: localize(turn, stage))

    transform(own - 1)

    def mem_copy(idx, stage):
        slots = pl.ds(2 * stage, 2)
        return remote(
            total.at[owned(idx, 1 - mem), slots], partner_part.at[idx, slots],
            mem_ss.at[idx, stage], mem_rs.at[idx, stage], partner,
        )

    for stage in range(stages - 1, -1, -1):
        localize(own - 1, stage)
        for idx in range(half):
            mem_copy(idx, stage).start()

    cutoff = col_count // 2 // 16 * 16
    bands = [slice(0, cutoff), slice(cutoff, col_count)]

    def lat_copy(idx, slot, band):
        rows = bands[band]
        return remote(
            lat_send.at[idx, slot, rows], lat_recv.at[idx, slot, rows],
            lat_ss.at[idx, slot, band], lat_rs.at[idx, slot, band],
            device(lax.rem(lat + lat_size - slot, lat_size), lon, mem),
        )

    def near_copy(idx, slot):
        return remote(
            near_send.at[idx, slot], near_recv.at[lax.rem(lon, half), slot],
            near_ss.at[idx, slot], near_rs.at[lax.rem(lon, half), slot],
            device(lax.rem(lat + lat_size - slot, lat_size), owned(quarter + idx, mem), mem),
        )

    slots = range(lat_size - 1, -1, -1)
    for idx in range(quarter):
        block = owned(idx, mem)
        for band in range(2):
            for slot in slots:
                if band == 0 and slot % 2 == 1:
                    mem_copy(idx, slot // 2).wait_recv()
                rows = bands[band]
                lat_send[idx, slot, rows] = (total[block, slot, rows] + partner_part[idx, slot, rows]).astype(bf16)
                if slot > 0:
                    lat_copy(idx, slot, band).start()
    for idx in range(quarter):
        block = owned(quarter + idx, mem)
        for slot in slots:
            if slot % 2 == 1:
                mem_copy(quarter + idx, slot // 2).wait_recv()
            value = (total[block, slot] + partner_part[quarter + idx, slot]).astype(bf16)
            if slot > 0:
                near_send[idx, slot] = value
                near_copy(idx, slot).start()
            else:
                @pl.when(block != lon)
                def _(idx=idx, value=value):
                    near_send[idx, 0] = value
                    near_copy(idx, 0).start()

                @pl.when(block == lon)
                def _(value=value):
                    near_recv[lax.rem(lon, half), 0] = value

    def lon_copy(idx, band):
        rows = bands[band]
        return remote(
            lon_send.at[idx, rows], lon_recv.at[lon, rows], lon_ss.at[idx, band], lon_rs.at[lon, band],
            device(lat, owned(idx, mem), mem),
        )

    for band in range(2):
        rows = bands[band]
        for idx in range(quarter):
            summed = lat_send[idx, 0, rows].astype(f32)
            for slot in range(1, lat_size):
                lat_copy(idx, slot, band).wait_recv()
                summed += lat_recv[idx, slot, rows].astype(f32)
            lon_send[idx, rows] = summed.astype(bf16)
            lon_copy(idx, band).start()

    def pair_copy(sender):
        return remote(lon_recv.at[sender], out.at[sender], pair_ss.at[sender], pair_rs.at[sender], partner)

    def out_copy(sender):
        return pltpu.make_async_copy(lon_recv.at[sender], out.at[sender], out_sem.at[sender])

    far = [(1 - side) * half + idx for idx in range(half)]
    close = [side * half + lax.rem(lon + idx, half) for idx in range(half)]

    @pl.when(receives)
    def _():
        for idx, sender in enumerate(close):
            local_level = lax.rem(lon + idx, half)
            summed = None
            for slot in range(lat_size):
                if idx + slot > 0:
                    remote(
                        near_send.at[0, slot], near_recv.at[local_level, slot], near_ss.at[0, slot],
                        near_rs.at[local_level, slot], device(lax.rem(lat + slot, lat_size), sender, mem),
                    ).wait_recv()
                term = near_recv[local_level, slot].astype(f32)
                summed = term if slot == 0 else summed + term
            lon_recv[sender] = summed.astype(bf16)
            pair_copy(sender).start()
            out_copy(sender).start()
        for sender in far:
            for band in range(2):
                rows = bands[band]
                remote(
                    lon_send.at[0, rows], lon_recv.at[sender, rows], lon_ss.at[0, band], lon_rs.at[sender, band],
                    device(lat, sender, mem),
                ).wait_recv()
            pair_copy(sender).start()
            out_copy(sender).start()

    @pl.when(jnp.logical_not(receives))
    def _():
        for sender in close + far:
            pair_copy(sender).wait_recv()

    @pl.when(receives)
    def _():
        for sender in close + far:
            pair_copy(sender).wait_send()
            out_copy(sender).wait()
        for slot in range(1, lat_size):
            gather_copy(slot).wait_send()
        for slot in range(lat_size):
            share_copy(slot).wait_send()

    for idx in range(half):
        for stage in range(stages):
            mem_copy(idx, stage).wait_send()
    for idx in range(quarter):
        for band in range(2):
            lon_copy(idx, band).wait_send()
            for slot in range(1, lat_size):
                lat_copy(idx, slot, band).wait_send()
        for slot in range(1, lat_size):
            near_copy(idx, slot).wait_send()
        pl.when(owned(quarter + idx, mem) != lon)(lambda idx=idx: near_copy(idx, 0).wait_send())
        pl.when(owned(quarter + idx, mem) != lon)(lambda idx=idx: innov_copy(idx).wait_send())
        far_copy(idx).wait_send()
    for step in range(1, lat_size):
        taper_copy(step).wait_send()
        trade_copy(step).wait_send()

    @pl.loop(0, own)
    def _(turn):
        for slot in range(lat_size):
            @pl.loop(1 if slot == 0 else 0, lon_size)
            def _(step, slot=slot):
                field_copy(turn, slot, step).wait_send()


def local(anomalies, taper, obs_row, obs_col, obs_level, obs_value):
    member_count, level_count, col_count, row_count = anomalies.shape
    lon_size, lat_size = lax.axis_size("lon"), lax.axis_size("lat")
    lat_total = row_count * lat_size
    ensemble = member_count * lax.axis_size("mem")
    own = member_count // lat_size
    half = lon_size // 2
    part_count = taper.shape[1]
    lon_total = col_count * lon_size
    seeds = lon_seeds(lon_total, lat_size) + lat_seeds(lat_total)
    share_pad = round_up(part_count // 4, 16)
    kind_size, points = lat_size * share_pad, round_up(lon_total // 4, 128)
    f32, bf16 = jnp.float32, jnp.bfloat16
    slab = (col_count, row_count)
    whole = pl.BlockSpec(memory_space=pl.ANY)
    dma = pltpu.SemaphoreType.DMA
    obs = [(table.shape, table.dtype) for table in (obs_level, obs_col, obs_row, obs_value)]
    near = obs + [(seed.shape, f32) for seed in seeds]
    result = pl.pallas_call(
        functools.partial(fused_kernel, lat_size, lon_size, own, obs_row.shape[0]),
        out_shape=jax.ShapeDtypeStruct((level_count,) + slab, bf16),
        in_specs=[whole] * 10,
        out_specs=whole,
        scratch_shapes=[
            pltpu.VMEM((own, lat_size, lon_size) + slab, bf16),
            pltpu.VMEM((2, kind_size, points), bf16),
            pltpu.VMEM((2 * kind_size, 2 * points), bf16),
            pltpu.VMEM((2, points, kind_size), bf16),
            pltpu.VMEM((2 * points, 2 * kind_size), bf16),
            pltpu.VMEM((points, 4 * kind_size), f32),
            pltpu.VMEM((lat_total, lat_total), bf16),
            pltpu.VMEM((part_count, lat_total), f32),
            pltpu.VMEM((4, lat_size, share_pad, lat_total), bf16),
            pltpu.VMEM((half // 2, 3) + obs_row.shape, bf16),
            pltpu.VMEM((half, 3) + obs_row.shape, bf16),
            pltpu.VMEM((3,) + obs_row.shape, f32),
            pltpu.VMEM(slab, f32),
            pltpu.VMEM((half // 2, col_count, 2 * row_count), f32),
            pltpu.VMEM((half // 2,) + slab, bf16),
            pltpu.VMEM((lat_size, lon_size) + slab, bf16),
            pltpu.VMEM((4 * points, 2 * row_count), bf16),
            pltpu.VMEM((4 * kind_size, 2 * row_count), bf16),
            pltpu.VMEM((4 * kind_size, lat_total), f32),
            pltpu.VMEM((4 * kind_size, lat_total), bf16),
            pltpu.VMEM((4 * kind_size, 2 * row_count), bf16),
            pltpu.VMEM((lon_size, lat_size) + slab, f32),
            pltpu.VMEM((half, lat_size) + slab, f32),
            pltpu.VMEM((half // 2, lat_size) + slab, bf16),
            pltpu.VMEM((half // 2, lat_size) + slab, bf16),
            pltpu.VMEM((half // 2, lat_size) + slab, bf16),
            pltpu.VMEM((half, lat_size) + slab, bf16),
            pltpu.VMEM((half // 2,) + slab, bf16),
            pltpu.VMEM((level_count,) + slab, bf16),
            *[pltpu.VMEM(shape, dtype) for shape, dtype in near],
            dma((own, lat_size, lon_size)), dma((own, lat_size, lon_size)), dma((own,)), dma((9,)),
            dma((lat_size,)), dma((lat_size,)), dma((lat_size,)), dma((lat_size,)),
            dma((half // 2,)), dma((half,)), dma((half // 2,)), dma((lon_size,)),
            dma((lat_size,)), dma((lat_size,)), dma((lat_size,)), dma((lat_size,)),
            dma((half, lat_size // 2)), dma((half, lat_size // 2)), dma((half // 2, lat_size, 2)),
            dma((half // 2, lat_size, 2)), dma((half // 2, lat_size)), dma((half, lat_size)),
            dma((half // 2, 2)), dma((lon_size, 2)), dma((lon_size,)), dma((lon_size,)), dma((lon_size,)),
        ],
        compiler_params=pltpu.CompilerParams(
            collective_id=0, has_side_effects=True, vmem_limit_bytes=60 * 1024 * 1024
        ),
    )(
        anomalies, taper, obs_level, obs_col, obs_row, obs_value, *seeds,
    )
    return result.astype(f32) / (ensemble - 1)


def solution(mesh):
    in_specs = (
        P("mem", None, "lon", "lat"),
        P("lon", "lat", None),
        P("lat", "lon"),
        P("lat", "lon"),
        P("lat", "lon"),
        P("lat", "lon"),
    )
    out_specs = P(None, "lon", "lat")
    return jax.shard_map(local, mesh=mesh, in_specs=in_specs, out_specs=out_specs, check_vma=False)
```
